512 devices in a mesh: gx: 4 (over x), gy: 8 (over y), gz: 16 (over z, core).
Axes of the slice: x: 4, y: 8, z: 8, core: 2. Of those that a mesh axis runs over, the one named last changes fastest.
Arguments:
- right_side: float32 [32, 128, 2048], P('gx', 'gy', 'gz'), may hold values from -6 to 6
- conductance: float32 [32, 128, 2048], P('gx', 'gy', 'gz'), may hold values from 0.25 to 4
- extents: int32 [4, 8, 16], P('gx', 'gy', 'gz'), may hold values from 64 to 128, as said below
- coarse_factor: bfloat16 [512, 512], replicated, may hold values from -1 to 3, as said below
Outputs:
- solution_field: float32 [32, 128, 2048], P('gx', 'gy', 'gz')
- residual: float32 [32, 128, 2048], P('gx', 'gy', 'gz')
The draws below stay inside these ranges and needn't reach their ends.
Inputs may be any that keep to these rules, and one draw needn't show every extreme that they name: `extents`: cells of a block whose third local index is below its count are fluid, the others padding; in every draw some block has all 128 layers fluid. `coarse_factor`: lower triangular with a positive diagonal.
All inputs are finite; a program needn't handle non-finite values.
Results may differ from the reference program's by a relative error of at most 0.0003.
Values sent between devices are 32-bit elements; how exact they have to be, the bound alone decides.
A program may use at most 64 MiB of HBM per device.

```python
import math
import jax
import jax.numpy as jnp
from jax import lax

CX = 8
CY = 16
CZ = 128
ITERS = 2
NX = 32
NY = 128
NZ = 2048
NB = 512
N_GX = 4
N_GY = 8
N_GZ = 16


def draw_right_side(key, part):
    key_cells, key_blocks = jax.random.split(jax.random.fold_in(key, 11), 2)
    blocks = (NX // CX, NY // CY, NZ // CZ)
    values = jnp.clip(jax.random.normal(key_cells, (NX, NY, NZ), jnp.float32), -4.0, 4.0)
    offsets = jax.random.uniform(key_blocks, blocks, jnp.float32, -1.5, 1.5)
    spread = jnp.repeat(jnp.repeat(jnp.repeat(offsets, CX, axis=0), CY, axis=1), CZ, axis=2)
    return values + spread


def draw_extents(key, part):
    key_counts, key_full = jax.random.split(jax.random.fold_in(key, 23))
    blocks = (NX // CX, NY // CY, NZ // CZ)
    counts = jax.random.randint(key_counts, blocks, CZ // 2, CZ + 1).reshape(-1)
    chosen = jax.random.randint(key_full, (), 0, counts.shape[0])
    counts = jnp.where(jnp.arange(counts.shape[0]) == chosen, CZ, counts)
    return counts.reshape(blocks).astype(jnp.int32)


def draw_coarse_factor(key, part):
    key_diag, key_low = jax.random.split(jax.random.fold_in(key, 37))
    diagonal = jax.random.uniform(key_diag, (NB,), jnp.float32, 1.0, 2.0)
    lower = jnp.clip(jax.random.normal(key_low, (NB, NB), jnp.float32), -6.0, 6.0)
    lower = jnp.tril(lower, -1) * (0.5 / math.sqrt(NB))
    return (lower + jnp.diag(diagonal)).astype(jnp.bfloat16)


def shard_levels(rng, shape, cuts, low, top_value):
    def one(axis_at, shards_of):
        steps = jax.random.uniform(jax.random.fold_in(jax.random.fold_in(rng, 6), axis_at), (shards_of,), jnp.float32, low / len(cuts), top_value / len(cuts))
        return jnp.repeat(jnp.exp(steps), shape[axis_at] // shards_of).reshape((-1,) + (1,) * (len(shape) - axis_at - 1))

    loudness = one(*cuts[0])
    for cut in cuts[1:]:
        loudness = loudness * one(*cut)
    return loudness


def setup_inputs(seed: int = 0) -> dict:
    streams_of = jax.random.split(jax.random.key(seed), 5)
    right_side = draw_right_side(jax.random.fold_in(streams_of[4], 71), 0)
    conductance = jnp.clip(jnp.exp(math.log(4.0) - 2.7725887 * jax.random.uniform(streams_of[1], (NX, NY, NZ), jnp.float32) ** shard_levels(streams_of[1], (NX, NY, NZ), ((0, 4), (1, 8), (2, 16)), -0.2, 0.2)), 0.25, 4.0)
    extents = draw_extents(jax.random.fold_in(streams_of[4], 71), 0)
    coarse_factor = draw_coarse_factor(jax.random.fold_in(streams_of[4], 71), 0)
    return dict(right_side=right_side, conductance=conductance, extents=extents, coarse_factor=coarse_factor)


OMEGA = 0.8

def neighbour_slices():
    inner = slice(1, -1)
    return [(slice(2, None), inner, inner), (slice(None, -2), inner, inner), (inner, slice(2, None), inner), (inner, slice(None, -2), inner), (inner, inner, slice(2, None)), (inner, inner, slice(None, -2))]

def face_terms(padded, cond_padded):
    centre = (slice(1, -1), slice(1, -1), slice(1, -1))
    value_mid = padded[centre]
    cond_mid = cond_padded[centre]
    summed = jnp.zeros_like(value_mid)
    for place in neighbour_slices():
        summed = summed + 0.5 * (cond_mid + cond_padded[place]) * (value_mid - padded[place])
    return summed

def coef_total(cond_padded):
    centre = (slice(1, -1), slice(1, -1), slice(1, -1))
    cond_mid = cond_padded[centre]
    summed = jnp.zeros_like(cond_mid)
    for place in neighbour_slices():
        summed = summed + 0.5 * (cond_mid + cond_padded[place])
    return summed

def pool_sum(field):
    first, second, third = field.shape
    return field.reshape(first // 2, 2, second // 2, 2, third // 2, 2).sum(axis=(1, 3, 5))

def pool_max(field):
    first, second, third = field.shape
    return field.reshape(first // 2, 2, second // 2, 2, third // 2, 2).max(axis=(1, 3, 5))

def expand(field):
    first, second, third = field.shape
    wide = jnp.broadcast_to(field[:, None, :, None, :, None], (first, 2, second, 2, third, 2))
    return wide.reshape(2 * first, 2 * second, 2 * third)

def make_level(cond_padded, fluid, scale):
    inverse = fluid / (scale * coef_total(cond_padded) + 1.0 - fluid)
    return (cond_padded, fluid, scale, inverse)

def apply_level(field, level):
    padded = jnp.pad(field, 1)
    return level[2] * level[1] * face_terms(padded, level[0])

def cycle(resid, levels, depth):
    level = levels[depth]
    first = OMEGA * level[3] * resid
    if depth == len(levels) - 1:
        return first
    image = apply_level(first, level)
    below = cycle(pool_sum(resid - image), levels, depth + 1)
    second = first + level[1] * expand(below)
    return second + OMEGA * level[3] * (resid - apply_level(second, level))

def reference(right_side, conductance, extents, coarse_factor):
    factor = coarse_factor.astype(jnp.float32)
    layer = lax.broadcasted_iota(jnp.int32, right_side.shape, 2) % CZ
    limit = jnp.repeat(jnp.repeat(jnp.repeat(extents, CX, axis=0), CY, axis=1), CZ, axis=2)
    fluid = (layer < limit).astype(jnp.float32)
    fluid_mid = pool_max(fluid)
    cond_mid = pool_sum(conductance) / 8.0
    levels = [make_level(jnp.pad(conductance, 1), fluid, 1.0), make_level(jnp.pad(cond_mid, 1), fluid_mid, 4.0)]
    block_cells = CX * CY * CZ

    def precondition(resid):
        smoothed = cycle(resid, levels, 0)
        means = resid.reshape(N_GX, CX, N_GY, CY, N_GZ, CZ).sum(axis=(1, 3, 5)).reshape(-1) / block_cells
        coarse = jax.scipy.linalg.cho_solve((factor, True), means)
        blockwise = coarse.reshape(N_GX, N_GY, N_GZ)
        spread = jnp.repeat(jnp.repeat(jnp.repeat(blockwise, CX, axis=0), CY, axis=1), CZ, axis=2)
        return smoothed + fluid * spread
    resid = fluid * right_side
    solution = jnp.zeros_like(resid)
    precond = precondition(resid)
    inner_now = jnp.sum(resid * precond)
    direction = precond
    for step in range(ITERS):
        image = apply_level(direction, levels[0])
        alpha = inner_now / jnp.sum(direction * image)
        solution = solution + alpha * direction
        resid = resid - alpha * image
        if step + 1 < ITERS:
            precond = precondition(resid)
            inner_next = jnp.sum(resid * precond)
            direction = precond + inner_next / inner_now * direction
            inner_now = inner_next
    return (solution, resid)
```

```python
import functools

import jax
import jax.numpy as jnp
from jax import lax
from jax.experimental import pallas as pl
from jax.experimental.pallas import tpu as pltpu
from jax.sharding import PartitionSpec as P

MESH = pl.DeviceIdType.MESH
HIGHEST = lax.Precision.HIGHEST
F32 = jnp.float32
NX, NR, NL = 24, 32, 128
SLOTS = [(dx, dy, dz) for dx in (-1, 0, 1) for dy in (-1, 0, 1) for dz in (-1, 0, 1)]
AROUND = [d for d in SLOTS if d != (0, 0, 0)]
PLANAR = [d for d in AROUND if d[2] == 0]
DEEP = [d for d in AROUND if d[2] != 0]


def slot(d):
    return (d[0] + 1) * 9 + (d[1] + 1) * 3 + d[2] + 1


def loop(low, high, unroll, body):
    whole = (high - low) // unroll

    def step(k, carry):
        for u in range(unroll):
            body(low + k * unroll + u)
        return carry

    if whole == 1:
        step(0, 0)
    else:
        lax.fori_loop(0, whole, step, 0)
    for i in range(low + whole * unroll, high):
        body(i)


def kernel(
    dims, rs_ref, c_ref, ext_ref, l_hbm, sol_ref, res_ref,
    R, C, WX, WY, WZ, INV, FI, SEC, V, D0, Q, D1, C1, INV1, F3, F13, FY3,
    KT, LB, YB, G, XT, ZS, ZR, RZ, RY, RX,
    l_sem, e_send, e_recv, x_send, x_recv, z_send, z_recv,
    gz_send, gz_recv, gy_send, gy_recv, gx_send, gx_recv,
):
    n_x, n_y, n_z = dims
    ix, iy, iz = (lax.axis_index(a) for a in ("gx", "gy", "gz"))

    def peer(dx, dy, dz):
        return {
            "gx": lax.rem(ix + dx + n_x, n_x),
            "gy": lax.rem(iy + dy + n_y, n_y),
            "gz": lax.rem(iz + dz + n_z, n_z),
        }

    l_copy = pltpu.make_async_copy(l_hbm, LB, l_sem)
    l_copy.start()

    greet = list(AROUND)
    greet += [(0, 0, o) for o in range(2, n_z - 1)]
    greet += [(0, o, 0) for o in range(2, n_y - 1)]
    greet += [(o, 0, 0) for o in range(2, n_x - 1)]
    barrier = pltpu.get_barrier_semaphore()
    for d in greet:
        pl.semaphore_signal(barrier, inc=1, device_id=peer(*d), device_id_type=MESH)

    lane = lax.broadcasted_iota(jnp.int32, (NR, NL), 1)
    sub = lax.broadcasted_iota(jnp.int32, (NR, NL), 0)
    last_lane, first_lane = lane == NL - 1, lane == 0
    even_z, even_y = lane % 2 == 0, sub % 2 == 0

    def yp(v):
        return pltpu.roll(v, NR - 1, 0)

    def ym(v):
        return pltpu.roll(v, 1, 0)

    def zp(p):
        a, b = pltpu.roll(p[0], NL - 1, 1), pltpu.roll(p[1], NL - 1, 1)
        return jnp.where(last_lane, b, a), jnp.where(last_lane, a, b)

    def zm(p):
        a, b = pltpu.roll(p[0], 1, 1), pltpu.roll(p[1], 1, 1)
        return jnp.where(first_lane, b, a), jnp.where(first_lane, a, b)

    def get(ref, i):
        return ref[i, 0:NR, :], ref[i, NR : 2 * NR, :]

    def put(ref, i, p):
        ref[i, 0:NR, :] = p[0]
        ref[i, NR : 2 * NR, :] = p[1]

    def each(f, *ps):
        return tuple(f(*(p[h] for p in ps)) for h in range(2))

    def pair_y(v):
        return v + jnp.where(even_y, yp(v), ym(v))

    def pair_z(v, op=jnp.add):
        return op(v, jnp.where(even_z, pltpu.roll(v, NL - 1, 1), pltpu.roll(v, 1, 1)))

    def fluid_of(i):
        return get(F3, i // 8)

    def a_plane(of, i, masked=True):
        v, vp, vm = of(i), of(i + 1), of(i - 1)
        wx, wxm, wy, wz = get(WX, i), get(WX, i - 1), get(WY, i), get(WZ, i)
        fy = each(lambda w, a: w * (a - yp(a)), wy, v)
        fz = each(lambda w, a, b: w * (a - b), wz, v, zp(v))
        fzm = zm(fz)
        out = each(
            lambda w, wm, a, ap, am, g, h, hm: w * (a - ap) + wm * (a - am) + (g - ym(g)) + (h - hm),
            wx, wxm, v, vp, vm, fy, fz, fzm,
        )
        if masked:
            out = each(jnp.multiply, fluid_of(i), out)
        return out

    def of(ref):
        return lambda i: get(ref, i)

    extent = jnp.full((1, NL), ext_ref[0, 0, 0].astype(F32))
    XT[13] = extent
    row16 = lax.broadcasted_iota(jnp.int32, (16, NL), 0)
    lane16 = lax.broadcasted_iota(jnp.int32, (16, NL), 1)
    own_fluid = (lane16.astype(F32) < extent).astype(F32)
    total = jnp.zeros((16, NL), F32)
    for i in range(8):
        r = own_fluid * rs_ref[i]
        R[8 + i, 0:16, :] = r
        total = total + r
        C[8 + i, 0:16, :] = c_ref[i]
    r_turned = R[8:16, 0:16, :].reshape(128, 128).T
    c_turned = c_ref[...].reshape(128, 128).T
    for h, at in ((0, 0), (1, 120)):
        ZS[h, 0] = r_turned[at : at + 8]
        ZS[h, 1] = c_turned[at : at + 8]
        ZS[h, 2] = jnp.broadcast_to(extent, (8, NL))

    izlo = lax.rem(iz, 8)

    def message(rows):
        t = jnp.zeros((16, NL), F32)
        for k, row in enumerate(rows):
            t = jnp.where(row16 == k, row, t)
        reduced = jnp.sum(t, axis=1, keepdims=True)
        placed = jnp.where(lane16 == row16 * 8 + izlo, reduced, 0.0)
        return jnp.sum(placed, axis=0, keepdims=True)

    def fold(v):
        return jnp.sum(v, axis=0, keepdims=True)

    pending = []

    def send(src, dst, s_sem, r_sem, to):
        copy = pltpu.make_async_remote_copy(
            src_ref=src, dst_ref=dst, send_sem=s_sem, recv_sem=r_sem,
            device_id=to, device_id_type=MESH,
        )
        copy.start()
        pending.append(copy)
        return copy

    def gather_z(g, row):
        RZ[g, iz] = row
        order = sorted(range(1, n_z), key=lambda o: -min(o, n_z - o))
        return [
            send(RZ.at[g, iz], RZ.at[g, iz], gz_send.at[g, o], gz_recv.at[g, o], peer(0, 0, o))
            for o in order
        ]

    def gather_y(g, before):
        for copy in before:
            copy.wait_recv()
        low, high = RZ[g, 0], RZ[g, 8]
        for k in range(1, 8):
            low, high = low + RZ[g, k], high + RZ[g, 8 + k]
        RY[g, iy, 0:1, :] = low
        RY[g, iy, 1:2, :] = high
        order = sorted(range(1, n_y), key=lambda o: -min(o, n_y - o))
        return [
            send(RY.at[g, iy], RY.at[g, iy], gy_send.at[g, o], gy_recv.at[g, o], peer(0, o, 0))
            for o in order
        ]

    def gather_x(g, before):
        for copy in before:
            copy.wait_recv()
        RX[g, ix] = RY[g]
        return [
            send(RY.at[g], RX.at[g, ix], gx_send.at[g, o], gx_recv.at[g, o], peer(o, 0, 0))
            for o in (2, 1, 3)
        ]

    def gathered(g, before):
        for copy in before:
            copy.wait_recv()
        for a in range(n_x):
            for b in range(n_y):
                at = (a * n_y + b) * 2
                G[at : at + 2, :] = RX[g, a, b]
        return G[...].T

    G[64:128, :] = jnp.zeros((64, NL), F32)
    first_row = message([fold(total)])
    pl.semaphore_wait(barrier, len(greet))

    stage = gather_z(0, first_row)

    incoming = []
    for d in PLANAR:
        dx, dy, _ = d
        to_x = {1: slice(0, 8), -1: slice(16, 24), 0: slice(8, 16)}[dx]
        from_y = {1: slice(8, 16), -1: slice(0, 8), 0: slice(0, 16)}[dy]
        to_y = {1: slice(24, 32), -1: slice(16, 24), 0: slice(0, 16)}[dy]
        back = slot((-dx, -dy, 0))
        k = slot(d)
        for f, ref in enumerate((C, R)):
            incoming.append(send(
                ref.at[8:16, from_y, :], ref.at[to_x, to_y, :],
                e_send.at[f, k], e_recv.at[f, k], peer(*d),
            ))
        incoming.append(send(XT.at[13], XT.at[back], x_send.at[k], x_recv.at[k], peer(*d)))
    for d in DEEP:
        dx, dy, dz = d
        k = slot(d)
        half = (dz + 1) // 2
        incoming.append(send(
            ZS.at[half], ZR.at[1 - half, (1 - dx) * 3 + 1 - dy],
            z_send.at[k], z_recv.at[k], peer(*d),
        ))

    l_copy.wait()
    KT[...] = jnp.zeros_like(KT)
    row = lax.broadcasted_iota(jnp.int32, (128, 128), 0)
    col = lax.broadcasted_iota(jnp.int32, (128, 128), 1)
    eye = row == col
    for b in range(4):
        at = slice(128 * b, 128 * b + 128)
        block = LB[at, at].astype(F32)
        KT[at, at] = jnp.where(eye, 1.0 / jnp.where(eye, block, 1.0), 0.0)

    def dot(a, b, turned=False):
        dims = (((1,), (1 if turned else 0,)), ((), ()))
        return lax.dot_general(a, b, dims, precision=HIGHEST, preferred_element_type=F32)

    def level(k, carry):
        r0, c0 = lax.shift_right_logical(row, k), lax.shift_right_logical(col, k)
        r1, c1 = lax.shift_right_logical(row, k + 1), lax.shift_right_logical(col, k + 1)
        mask = (r1 == c1) & (r0 > c0)
        for b in range(4):
            at = slice(128 * b, 128 * b + 128)
            m = jnp.where(mask, LB[at, at].astype(F32), 0.0)
            kt = KT[at, at]
            KT[at, at] = kt - dot(dot(kt, m, True), kt)
        return carry

    lax.fori_loop(0, 7, level, 0)

    stage = gather_y(0, stage)

    def join(a, b, w):
        up, down = slice(a, a + w), slice(b, b + w)
        l = LB[down, up].astype(F32)
        KT[up, down] = -dot(dot(KT[up, up], l, True), KT[down, down])

    join(0, 128, 128)
    join(256, 384, 128)
    join(0, 256, 256)

    for copy in incoming:
        copy.wait_recv()

    def there(dx, dy, dz):
        ok = None
        for d, i, n in ((dx, ix, n_x), (dy, iy, n_y), (dz, iz, n_z)):
            if d:
                test = i + d >= 0 if d < 0 else i + d < n
                ok = test if ok is None else ok & test
        return jnp.float32(1.0) if ok is None else ok.astype(F32)

    def blockwise(value, dx):
        lower = sub < 16
        upper = sub < 24
        near = [value(dx, dy, 0) for dy in (0, 1, -1)]
        above = [value(dx, dy, 1) for dy in (0, 1, -1)]
        below = [value(dx, dy, -1) for dy in (0, 1, -1)]
        by_y = [jnp.where(lower, a, jnp.where(upper, b, c)) for a, b, c in (near, above, below)]
        return by_y[0], jnp.where(lane < 64, by_y[1], by_y[2])

    def extent_at(dx, dy, dz):
        if dz == 0:
            e = XT[slot((dx, dy, dz))]
        else:
            e = ZR[(dz + 1) // 2, (dx + 1) * 3 + dy + 1, 2, 0:1, :]
        return e * there(dx, dy, dz)

    lane_f = lane.astype(F32)
    for dx in (-1, 0, 1):
        f = each(lambda e: (lane_f < e).astype(F32), blockwise(extent_at, dx))
        put(F3, dx + 1, f)
        put(F13, dx + 1, each(lambda a: pair_z(a, jnp.maximum), f))

    blank = jnp.zeros((104 + 8, NL), F32)
    for dx in (-1, 0, 1):
        to_x = 8 + 8 * dx
        for dy in (-1, 0, 1):
            from_y = {1: 0, -1: 8, 0: 0}[dy]
            to_y = {1: 16, -1: 24, 0: 0}[dy]
            wide = 16 if dy == 0 else 8
            at = (dx + 1) * 3 + dy + 1
            above, below = there(dx, dy, 1), there(dx, dy, -1)
            for f, ref in enumerate((R, C)):
                t = jnp.concatenate([ZR[1, at, f] * above, blank, ZR[0, at, f] * below], axis=0).T
                t = t.reshape(8, 16, NL)
                ref[to_x : to_x + 8, NR + to_y : NR + to_y + wide, :] = t[:, from_y : from_y + wide, :]

    @pl.when(ix == 0)
    def _():
        C[0:8, 0:NR, :] = jnp.zeros((8, NR, NL), F32)

    @pl.when(ix == n_x - 1)
    def _():
        C[16:24, 0:NR, :] = jnp.zeros((8, NR, NL), F32)

    @pl.when(iy == n_y - 1)
    def _():
        C[:, 16:24, :] = jnp.zeros((NX, 8, NL), F32)

    @pl.when(iy == 0)
    def _():
        C[:, 24:32, :] = jnp.zeros((NX, 8, NL), F32)

    def coefficients(i):
        c, cp, cm = get(C, i), get(C, i + 1), get(C, i - 1)
        half = lambda a, b: 0.5 * (a + b)
        wx, wxm = each(half, c, cp), each(half, c, cm)
        wy = each(lambda a: half(a, yp(a)), c)
        wz = each(half, c, zp(c))
        f = fluid_of(i)
        inv = each(
            lambda a, am, b, z, m, g: 0.8 * g / (a + am + b + ym(b) + z + m + 1.0 - g),
            wx, wxm, wy, wz, zm(wz), f,
        )
        put(WX, i, wx)
        put(WY, i, wy)
        put(WZ, i, wz)
        put(INV, i, inv)
        put(FI, i, each(jnp.multiply, inv, get(R, i)))

    loop(1, 23, 2, coefficients)

    def pool(a, b):
        return each(lambda u, v: pair_z(pair_y(u + v)), a, b)

    def coarse_mean(j):
        put(C1, j, each(lambda a: a * 0.125, pool(get(C, 2 * j), get(C, 2 * j + 1))))

    loop(0, 12, 2, coarse_mean)
    near_end, near_start = lane >= NL - 2, lane < 2

    def coarse_inverse(j):
        c = get(C1, j)
        f = get(F13, j // 4)
        u = [pltpu.roll(v, NL - 2, 1) for v in c]
        d = [pltpu.roll(v, 2, 1) for v in c]
        up = (jnp.where(near_end, u[1], u[0]), jnp.where(near_end, u[0], u[1]))
        down = (jnp.where(near_start, d[1], d[0]), jnp.where(near_start, d[0], d[1]))
        put(INV1, j, each(
            lambda a, p, m, g, h, e: 0.8 * e / (
                2.0 * (6.0 * a + p + m + pltpu.roll(a, NR - 2, 0) + pltpu.roll(a, 2, 0) + g + h) + 1.0 - e
            ),
            c, get(C1, j + 1), get(C1, j - 1), up, down, f,
        ))

    loop(1, 11, 2, coarse_inverse)

    def correct(src, low, high):
        def body(j):
            rest = [
                each(jnp.subtract, get(src, i), a_plane(of(FI), i)) for i in (2 * j, 2 * j + 1)
            ]
            below = each(jnp.multiply, get(INV1, j), pool(*rest))
            shift = each(jnp.multiply, get(F3, j // 4), below)
            for i in (2 * j, 2 * j + 1):
                put(SEC, i, each(jnp.add, get(FI, i), shift))

        loop(low, high, 1, body)

    def smooth(src, dst, low, high):
        def body(i):
            put(dst, i, each(
                lambda s, w, r, a: s + w * (r - a),
                get(SEC, i), get(INV, i), get(src, i), a_plane(of(SEC), i),
            ))

        loop(low, high, 2, body)

    stage = gather_x(0, stage)
    correct(R, 1, 11)
    smooth(R, D0, 4, 20)

    def own_sum(p):
        return p[0][0:16]

    def coupling(i, carry):
        e, kz = carry
        f, fn = get(F3, 1), zp(get(F3, 1))
        e = e + own_sum(a_plane(fluid_of, i))
        kz = kz + jnp.where(lane16 == NL - 1, WZ[i, 0:16, :] * f[0][0:16] * fn[0][0:16], 0.0)
        return e, kz

    zero16 = jnp.zeros((16, NL), F32)
    e_part, kz_part = lax.fori_loop(8, 16, coupling, (zero16, zero16))
    kx_part = WX[15, 0:16, :] * F3[1, 0:16, :] * F3[2, 0:16, :]
    ky_part = WY[8, 15:16, :]
    for i in range(9, 16):
        ky_part = ky_part + WY[i, 15:16, :]
    ky_part = ky_part * F3[1, 15:16, :] * F3[1, 16:17, :]

    lane8 = lax.broadcasted_iota(jnp.int32, (8, NL), 1)
    sub8 = lax.broadcasted_iota(jnp.int32, (8, NL), 0)

    def solve(m):
        parts = [[jnp.zeros((8, NL), F32) for _ in range(2)] for _ in range(4)]
        for l in range(64):
            value = jnp.broadcast_to(m[:, l : l + 1], (8, NL))
            for c in range(l // 16, 4):
                parts[c][l % 2] += value * KT[8 * l : 8 * l + 8, NL * c : NL * c + NL]
        t = [jnp.broadcast_to(fold(a + b), (8, NL)) for a, b in parts]
        y = jnp.zeros((8, NL), F32)
        for l in range(64):
            p = None
            for c in range(l // 16, 4):
                q = t[c] * KT[8 * l : 8 * l + 8, NL * c : NL * c + NL]
                p = q if p is None else p + q
            s = jnp.broadcast_to(jnp.sum(p, axis=1, keepdims=True), (8, NL))
            YB[8 * l : 8 * l + 8, :] = s
            y = jnp.where(lane8 == l, s, y)
        return y

    def y_at(dx, dy, dz):
        def held(i, d, n):
            return jnp.clip(i + d, 0, n - 1)

        b = (held(ix, dx, n_x) * n_y + held(iy, dy, n_y)) * n_z + held(iz, dz, n_z)
        return YB[pl.ds(b, 1), :]

    def spread():
        for dx in (-1, 0, 1):
            put(FY3, dx + 1, each(jnp.multiply, get(F3, dx + 1), blockwise(y_at, dx)))

    sums0 = gathered(0, stage)[0:8]
    solve(sums0 * (1.0 / 16384.0))
    spread()

    def add_coarse(i):
        put(D0, i, each(jnp.add, get(D0, i), get(FY3, i // 8)))

    loop(4, 20, 4, add_coarse)

    def first_image(i):
        q = a_plane(of(D0), i)
        put(Q, i, q)
        put(FI, i, each(jnp.multiply, get(INV, i), q))

    loop(5, 19, 2, first_image)
    correct(Q, 3, 9)
    smooth(Q, V, 7, 17)

    def products(i, carry):
        r, d, q, v = (ref[i, 0:16, :] for ref in (R, D0, Q, V))
        w = own_sum(a_plane(of(V), i))
        new = (r * d, d * q, q, r * v, q * v, v * w, w)
        return tuple(a + b for a, b in zip(carry, new))

    parts = lax.fori_loop(8, 16, products, (zero16,) * 7)
    rows = [fold(p) for p in parts]
    rows += [fold(e_part), fold(kx_part), ky_part, fold(kz_part)]
    stage = gather_z(1, message(rows))
    stage = gather_y(1, stage)
    stage = gather_x(1, stage)
    turned = gathered(1, stage)
    rd, dq, q_sum, rv, qv, vw, w_sum, e_all, kx, ky, kz = (
        turned[8 * k : 8 * k + 8] for k in range(11)
    )
    y = solve(q_sum * (1.0 / 16384.0))
    spread()

    def all_sum(v):
        return jnp.sum(jnp.sum(v, axis=0, keepdims=True), axis=1, keepdims=True)

    up = pltpu.roll(y, 7, 0)
    y_z = jnp.where(sub8 == 7, pltpu.roll(up, NL - 1, 1), up)
    y_y = pltpu.roll(y, NL - 2, 1)
    y_x = pltpu.roll(y, NL - 16, 1)
    jump = kx * (y - y_x) ** 2 + ky * (y - y_y) ** 2 + kz * (y - y_z) ** 2
    p1, p2 = all_sum(rd), all_sum(dq)
    p4 = all_sum(rv + sums0 * y)
    p5 = all_sum(qv + q_sum * y)
    p6 = all_sum(vw + 2.0 * y * w_sum + e_all * y * y + jump)
    alpha = p1 / p2
    inner = p1 - alpha * (p4 + p2) + alpha * alpha * p5
    ratio = inner / p1
    grown = 1.0 + ratio
    curve = grown * grown * p2 - 2.0 * grown * alpha * p5 + alpha * alpha * p6
    alpha2 = inner / curve

    def direction(i):
        put(D1, i, each(
            lambda d, v, s: grown * d - alpha * (v + s), get(D0, i), get(V, i), get(FY3, i // 8)
        ))

    loop(7, 17, 2, direction)

    def finish(i):
        d0, d1, r, q = (ref[i, 0:16, :] for ref in (D0, D1, R, Q))
        image = own_sum(a_plane(of(D1), i))
        sol_ref[i - 8] = alpha * d0 + alpha2 * d1
        res_ref[i - 8] = r - alpha * q - alpha2 * image

    loop(8, 16, 2, finish)

    for copy in pending:
        copy.wait_send()


def solution(mesh):
    dims = tuple(mesh.shape[a] for a in ("gx", "gy", "gz"))
    field = pltpu.VMEM((NX, 2 * NR, NL), F32)
    coarse = pltpu.VMEM((NX // 2, 2 * NR, NL), F32)
    three = pltpu.VMEM((3, 2 * NR, NL), F32)
    sems = pltpu.SemaphoreType.DMA

    def on_device(right_side, conductance, extents, coarse_factor):
        shape = jax.ShapeDtypeStruct((8, 16, 128), F32)
        return pl.pallas_call(
            functools.partial(kernel, dims),
            out_shape=(shape, shape),
            in_specs=[
                pl.BlockSpec(memory_space=pltpu.VMEM),
                pl.BlockSpec(memory_space=pltpu.VMEM),
                pl.BlockSpec(memory_space=pltpu.SMEM),
                pl.BlockSpec(memory_space=pl.ANY),
            ],
            out_specs=(
                pl.BlockSpec(memory_space=pltpu.VMEM),
                pl.BlockSpec(memory_space=pltpu.VMEM),
            ),
            scratch_shapes=[
                *([field] * 12), coarse, coarse, three, three, three,
                pltpu.VMEM((512, 512), F32),
                pltpu.VMEM((512, 512), jnp.bfloat16),
                pltpu.VMEM((512, NL), F32),
                pltpu.VMEM((NL, NL), F32),
                pltpu.VMEM((27, 1, NL), F32),
                pltpu.VMEM((2, 3, 8, NL), F32),
                pltpu.VMEM((2, 9, 3, 8, NL), F32),
                pltpu.VMEM((2, 16, 1, NL), F32),
                pltpu.VMEM((2, 8, 2, NL), F32),
                pltpu.VMEM((2, 4, 8, 2, NL), F32),
                sems(()),
                sems((2, 27)), sems((2, 27)),
                sems((27,)), sems((27,)),
                sems((27,)), sems((27,)),
                sems((2, 16)), sems((2, 16)),
                sems((2, 8)), sems((2, 8)),
                sems((2, 4)), sems((2, 4)),
            ],
            compiler_params=pltpu.CompilerParams(collective_id=0, has_side_effects=True),
        )(right_side, conductance, extents, coarse_factor)

    spec = P("gx", "gy", "gz")
    return jax.shard_map(
        on_device, mesh=mesh, in_specs=(spec, spec, spec, P()), out_specs=(spec, spec),
        check_vma=False,
    )
```

```python
import functools

import jax
import jax.numpy as jnp
from jax import lax
from jax.experimental import pallas as pl
from jax.experimental.pallas import tpu as pltpu
from jax.sharding import PartitionSpec as P

MESH = pl.DeviceIdType.MESH
F32, BF16 = jnp.float32, jnp.bfloat16
NX, NR, NL = 24, 32, 128
SLOTS = [(dx, dy, dz) for dx in (-1, 0, 1) for dy in (-1, 0, 1) for dz in (-1, 0, 1)]
AROUND = [d for d in SLOTS if d != (0, 0, 0)]
PLANAR = [d for d in AROUND if d[2] == 0]
DEEP = [d for d in AROUND if d[2] != 0]


def slot(d):
    return (d[0] + 1) * 9 + (d[1] + 1) * 3 + d[2] + 1


def dot(a, b, turned=False):
    dims = (((1,), (1 if turned else 0,)), ((), ()))
    return lax.dot_general(a, b, dims, preferred_element_type=F32)


def three(x):
    a = x.astype(BF16)
    rest = x - a.astype(F32)
    b = rest.astype(BF16)
    return a, b, (rest - b.astype(F32)).astype(BF16)


def dot_turned(x, m):
    n = x.shape[0]
    p = dot(jnp.concatenate(three(x), axis=0), m, True)
    return p[0:n] + (p[n : 2 * n] + p[2 * n :])


def dot_wide(x, y):
    n = x.shape[0]
    (a, b, c), (d, e, f) = three(x), three(y)
    p = dot(jnp.concatenate([a, b, c], axis=0), d)
    q = dot(jnp.concatenate([a, b], axis=0), e)
    return p[0:n] + ((p[n : 2 * n] + q[0:n]) + (p[2 * n :] + q[n:] + dot(a, f)))


def loop(low, high, unroll, body):
    whole = (high - low) // unroll

    def step(k, carry):
        for u in range(unroll):
            body(low + k * unroll + u)
        return carry

    if whole == 1:
        step(0, 0)
    else:
        lax.fori_loop(0, whole, step, 0)
    for i in range(low + whole * unroll, high):
        body(i)


def kernel(
    dims, rs_ref, c_ref, ext_ref, l_hbm, sol_ref, res_ref,
    R, C, WX, WY, WZ, INV, FI, SEC, V, D0, Q, D1, C1, INV1, F3, F13, FY3,
    KT, LB, YB, G, XT, ZS, ZR, RZ, RY, RX, MX, MY, MZ,
    l_sem, send_sem, recv_sem,
):
    n_x, n_y, n_z = dims
    ix, iy, iz = (lax.axis_index(a) for a in ("gx", "gy", "gz"))

    def peer(dx, dy, dz):
        return {
            "gx": lax.rem(ix + dx + n_x, n_x),
            "gy": lax.rem(iy + dy + n_y, n_y),
            "gz": lax.rem(iz + dz + n_z, n_z),
        }

    l_copy = pltpu.make_async_copy(l_hbm, LB, l_sem)
    l_copy.start()

    greet = list(AROUND)
    greet += [(0, 0, o) for o in range(2, n_z - 1)]
    greet += [(0, o, 0) for o in range(2, n_y - 1)]
    greet += [(o, 0, 0) for o in range(2, n_x - 1)]
    barrier = pltpu.get_barrier_semaphore()
    for d in greet:
        pl.semaphore_signal(barrier, inc=1, device_id=peer(*d), device_id_type=MESH)

    lane = lax.broadcasted_iota(jnp.int32, (NR, NL), 1)
    sub = lax.broadcasted_iota(jnp.int32, (NR, NL), 0)
    last_lane, first_lane = lane == NL - 1, lane == 0
    even_z, even_y = lane % 2 == 0, sub % 2 == 0

    def yp(v):
        return pltpu.roll(v, NR - 1, 0)

    def ym(v):
        return pltpu.roll(v, 1, 0)

    def zp(p):
        a, b = pltpu.roll(p[0], NL - 1, 1), pltpu.roll(p[1], NL - 1, 1)
        return jnp.where(last_lane, b, a), jnp.where(last_lane, a, b)

    def zm(p):
        a, b = pltpu.roll(p[0], 1, 1), pltpu.roll(p[1], 1, 1)
        return jnp.where(first_lane, b, a), jnp.where(first_lane, a, b)

    def get(ref, i):
        return ref[i, 0:NR, :], ref[i, NR : 2 * NR, :]

    def put(ref, i, p):
        ref[i, 0:NR, :] = p[0]
        ref[i, NR : 2 * NR, :] = p[1]

    def each(f, *ps):
        return tuple(f(*(p[h] for p in ps)) for h in range(2))

    def pair_y(v):
        return v + jnp.where(even_y, yp(v), ym(v))

    def pair_z(v, op=jnp.add):
        return op(v, jnp.where(even_z, pltpu.roll(v, NL - 1, 1), pltpu.roll(v, 1, 1)))

    def fluid_of(i):
        return get(F3, i // 8)

    def a_plane(of, i, masked=True):
        v, vp, vm = of(i), of(i + 1), of(i - 1)
        wx, wxm, wy, wz = get(WX, i), get(WX, i - 1), get(WY, i), get(WZ, i)
        fy = each(lambda w, a: w * (a - yp(a)), wy, v)
        fz = each(lambda w, a, b: w * (a - b), wz, v, zp(v))
        fzm = zm(fz)
        out = each(
            lambda w, wm, a, ap, am, g, h, hm: w * (a - ap) + wm * (a - am) + (g - ym(g)) + (h - hm),
            wx, wxm, v, vp, vm, fy, fz, fzm,
        )
        if masked:
            out = each(jnp.multiply, fluid_of(i), out)
        return out

    def of(ref):
        return lambda i: get(ref, i)

    extent = jnp.full((1, NL), ext_ref[0, 0, 0].astype(F32))
    XT[13] = extent
    row16 = lax.broadcasted_iota(jnp.int32, (16, NL), 0)
    lane16 = lax.broadcasted_iota(jnp.int32, (16, NL), 1)
    own_fluid = (lane16.astype(F32) < extent).astype(F32)
    total = jnp.zeros((16, NL), F32)
    for i in range(8):
        r = own_fluid * rs_ref[i]
        R[8 + i, 0:16, :] = r
        total = total + r
        C[8 + i, 0:16, :] = c_ref[i]

    izlo = lax.rem(iz, 8)

    def message(rows):
        t = jnp.zeros((16, NL), F32)
        for k, row in enumerate(rows):
            t = jnp.where(row16 == k, row, t)
        reduced = jnp.sum(t, axis=1, keepdims=True)
        placed = jnp.where(lane16 == row16 * 8 + izlo, reduced, 0.0)
        return jnp.sum(placed, axis=0, keepdims=True)

    def fold(v):
        return jnp.sum(v, axis=0, keepdims=True)

    pending = []

    def send(src, dst, group, to):
        pltpu.make_async_remote_copy(
            src_ref=src, dst_ref=dst, send_sem=send_sem.at[group], recv_sem=recv_sem.at[group],
            device_id=to, device_id_type=MESH,
        ).start()

    def take(sem, all_bytes):
        pltpu.make_async_copy(all_bytes, all_bytes, sem).wait()

    def arrived(group, all_bytes):
        take(recv_sem.at[group], all_bytes)
        pending.append((group, all_bytes))

    def far_first(n):
        return sorted(range(1, n), key=lambda o: -min(o, n - o))

    def row_stage(group, ref, at, row, n, direction):
        ref[at] = row
        for o in far_first(n):
            send(ref.at[at], ref.at[at], group, peer(*direction(o)))

    def added(ref, n):
        row = ref[0]
        for k in range(1, n):
            row = row + ref[k]
        return row

    def gather(row):
        row_stage(3, RZ, iz, row, n_z, lambda o: (0, 0, o))
        arrived(3, RZ.at[0 : n_z - 1])
        low, high = RZ[0], RZ[8]
        for k in range(1, 8):
            low, high = low + RZ[k], high + RZ[8 + k]
        RY[iy, 0:1, :] = low
        RY[iy, 1:2, :] = high
        for o in far_first(n_y):
            send(RY.at[iy], RY.at[iy], 4, peer(0, o, 0))
        arrived(4, RY.at[0 : n_y - 1])
        RX[ix] = RY[...]
        for o in far_first(n_x):
            send(RY, RX.at[ix], 5, peer(o, 0, 0))
        arrived(5, RX.at[0 : n_x - 1])
        for a in range(n_x):
            for b in range(n_y):
                at = (a * n_y + b) * 2
                G[at : at + 2, :] = RX[a, b]
        return G[...].T

    column = (ix * n_y + iy) * 2 + iz // 8
    lane1 = lax.broadcasted_iota(jnp.int32, (1, NL), 1)
    first_row = jnp.where(lane1 == column, jnp.sum(fold(total), axis=1, keepdims=True), 0.0)
    pl.semaphore_wait(barrier, len(greet))
    row_stage(0, MX, ix, first_row, n_x, lambda o: (o, 0, 0))

    for d in PLANAR:
        dx, dy, _ = d
        to_x = {1: slice(0, 8), -1: slice(16, 24), 0: slice(8, 16)}[dx]
        from_y = {1: slice(8, 16), -1: slice(0, 8), 0: slice(0, 16)}[dy]
        to_y = {1: slice(24, 32), -1: slice(16, 24), 0: slice(0, 16)}[dy]
        for group, ref in ((6, C), (7, R)):
            send(ref.at[8:16, from_y, :], ref.at[to_x, to_y, :], group, peer(*d))
        send(XT.at[13], XT.at[slot((-dx, -dy, 0))], 8, peer(*d))
    r_turned = R[8:16, 0:16, :].reshape(128, 128).T
    c_turned = c_ref[...].reshape(128, 128).T
    for h, at in ((0, 0), (1, 120)):
        ZS[h, 0] = r_turned[at : at + 8]
        ZS[h, 1] = c_turned[at : at + 8]
        ZS[h, 2] = jnp.broadcast_to(extent, (8, NL))
    for d in DEEP:
        dx, dy, dz = d
        half = (dz + 1) // 2
        send(ZS.at[half], ZR.at[1 - half, (1 - dx) * 3 + 1 - dy], 9, peer(*d))

    l_copy.wait()
    KT[...] = jnp.zeros_like(KT)
    row = lax.broadcasted_iota(jnp.int32, (128, 128), 0)
    col = lax.broadcasted_iota(jnp.int32, (128, 128), 1)
    eye = row == col
    for b in range(4):
        at = slice(128 * b, 128 * b + 128)
        block = LB[at, at].astype(F32)
        KT[at, at] = jnp.where(eye, 1.0 / jnp.where(eye, block, 1.0), 0.0)

    def level(k):
        mask = (row // (2 << k) == col // (2 << k)) & (row // (1 << k) > col // (1 << k))
        for b in range(4):
            at = slice(128 * b, 128 * b + 128)
            m = jnp.where(mask, LB[at, at].astype(F32), 0.0).astype(BF16)
            kt = KT[at, at]
            KT[at, at] = kt - dot_wide(dot_turned(kt, m), kt)

    def join(a, b, w):
        up, down = slice(a, a + w), slice(b, b + w)
        KT[up, down] = -dot_wide(dot_turned(KT[up, up], LB[down, up]), KT[down, down])

    for k in range(4):
        level(k)
    arrived(0, MX.at[0 : n_x - 1])
    row_stage(1, MY, iy, added(MX, n_x), n_y, lambda o: (0, o, 0))
    for k in range(4, 7):
        level(k)
    join(0, 128, 128)
    join(256, 384, 128)
    join(0, 256, 256)
    G[64:128, :] = jnp.zeros((64, NL), F32)
    arrived(1, MY.at[0 : n_y - 1])
    row_stage(2, MZ, iz, added(MY, n_y), n_z, lambda o: (0, 0, o))

    arrived(6, C.at[0:10])
    arrived(7, R.at[0:10])
    arrived(8, XT.at[0:8])
    arrived(9, ZR)

    def there(dx, dy, dz):
        ok = None
        for d, i, n in ((dx, ix, n_x), (dy, iy, n_y), (dz, iz, n_z)):
            if d:
                test = i + d >= 0 if d < 0 else i + d < n
                ok = test if ok is None else ok & test
        return jnp.float32(1.0) if ok is None else ok.astype(F32)

    def blockwise(value, dx):
        lower = sub < 16
        upper = sub < 24
        near = [value(dx, dy, 0) for dy in (0, 1, -1)]
        above = [value(dx, dy, 1) for dy in (0, 1, -1)]
        below = [value(dx, dy, -1) for dy in (0, 1, -1)]
        by_y = [jnp.where(lower, a, jnp.where(upper, b, c)) for a, b, c in (near, above, below)]
        return by_y[0], jnp.where(lane < 64, by_y[1], by_y[2])

    def extent_at(dx, dy, dz):
        if dz == 0:
            e = XT[slot((dx, dy, dz))]
        else:
            e = ZR[(dz + 1) // 2, (dx + 1) * 3 + dy + 1, 2, 0:1, :]
        return e * there(dx, dy, dz)

    lane_f = lane.astype(F32)
    for dx in (-1, 0, 1):
        f = each(lambda e: (lane_f < e).astype(F32), blockwise(extent_at, dx))
        put(F3, dx + 1, f)
        put(F13, dx + 1, each(lambda a: pair_z(a, jnp.maximum), f))

    blank = jnp.zeros((104 + 8, NL), F32)
    for dx in (-1, 0, 1):
        to_x = 8 + 8 * dx
        for dy in (-1, 0, 1):
            from_y = {1: 0, -1: 8, 0: 0}[dy]
            to_y = {1: 16, -1: 24, 0: 0}[dy]
            wide = 16 if dy == 0 else 8
            at = (dx + 1) * 3 + dy + 1
            above, below = there(dx, dy, 1), there(dx, dy, -1)
            for f, ref in enumerate((R, C)):
                t = jnp.concatenate([ZR[1, at, f] * above, blank, ZR[0, at, f] * below], axis=0).T
                t = t.reshape(8, 16, NL)
                ref[to_x : to_x + 8, NR + to_y : NR + to_y + wide, :] = t[:, from_y : from_y + wide, :]

    @pl.when(ix == 0)
    def _():
        C[0:8, 0:NR, :] = jnp.zeros((8, NR, NL), F32)

    @pl.when(ix == n_x - 1)
    def _():
        C[16:24, 0:NR, :] = jnp.zeros((8, NR, NL), F32)

    @pl.when(iy == n_y - 1)
    def _():
        C[:, 16:24, :] = jnp.zeros((NX, 8, NL), F32)

    @pl.when(iy == 0)
    def _():
        C[:, 24:32, :] = jnp.zeros((NX, 8, NL), F32)

    def coefficients(i):
        c, cp, cm = get(C, i), get(C, i + 1), get(C, i - 1)
        half = lambda a, b: 0.5 * (a + b)
        wx, wxm = each(half, c, cp), each(half, c, cm)
        wy = each(lambda a: half(a, yp(a)), c)
        wz = each(half, c, zp(c))
        f = fluid_of(i)
        inv = each(
            lambda a, am, b, z, m, g: 0.8 * g / (a + am + b + ym(b) + z + m + 1.0 - g),
            wx, wxm, wy, wz, zm(wz), f,
        )
        put(WX, i, wx)
        put(WY, i, wy)
        put(WZ, i, wz)
        put(INV, i, inv)
        put(FI, i, each(jnp.multiply, inv, get(R, i)))

    loop(1, 23, 2, coefficients)

    def pool(a, b):
        return each(lambda u, v: pair_z(pair_y(u + v)), a, b)

    def coarse_mean(j):
        put(C1, j, each(lambda a: a * 0.125, pool(get(C, 2 * j), get(C, 2 * j + 1))))

    loop(0, 12, 2, coarse_mean)
    near_end, near_start = lane >= NL - 2, lane < 2

    def coarse_inverse(j):
        c = get(C1, j)
        f = get(F13, j // 4)
        u = [pltpu.roll(v, NL - 2, 1) for v in c]
        d = [pltpu.roll(v, 2, 1) for v in c]
        up = (jnp.where(near_end, u[1], u[0]), jnp.where(near_end, u[0], u[1]))
        down = (jnp.where(near_start, d[1], d[0]), jnp.where(near_start, d[0], d[1]))
        put(INV1, j, each(
            lambda a, p, m, g, h, e: 0.8 * e / (
                2.0 * (6.0 * a + p + m + pltpu.roll(a, NR - 2, 0) + pltpu.roll(a, 2, 0) + g + h) + 1.0 - e
            ),
            c, get(C1, j + 1), get(C1, j - 1), up, down, f,
        ))

    loop(1, 11, 2, coarse_inverse)

    def correct(src, low, high):
        def body(j):
            rest = [
                each(jnp.subtract, get(src, i), a_plane(of(FI), i)) for i in (2 * j, 2 * j + 1)
            ]
            below = each(jnp.multiply, get(INV1, j), pool(*rest))
            shift = each(jnp.multiply, get(F3, j // 4), below)
            for i in (2 * j, 2 * j + 1):
                put(SEC, i, each(jnp.add, get(FI, i), shift))

        loop(low, high, 1, body)

    def smooth(src, dst, low, high):
        def body(i):
            put(dst, i, each(
                lambda s, w, r, a: s + w * (r - a),
                get(SEC, i), get(INV, i), get(src, i), a_plane(of(SEC), i),
            ))

        loop(low, high, 2, body)

    correct(R, 1, 11)
    smooth(R, D0, 4, 20)

    def own_sum(p):
        return p[0][0:16]

    def coupling(i, carry):
        e, kz = carry
        f, fn = get(F3, 1), zp(get(F3, 1))
        e = e + own_sum(a_plane(fluid_of, i))
        kz = kz + jnp.where(lane16 == NL - 1, WZ[i, 0:16, :] * f[0][0:16] * fn[0][0:16], 0.0)
        return e, kz

    zero16 = jnp.zeros((16, NL), F32)
    e_part, kz_part = lax.fori_loop(8, 16, coupling, (zero16, zero16))
    kx_part = WX[15, 0:16, :] * F3[1, 0:16, :] * F3[2, 0:16, :]
    ky_part = WY[8, 15:16, :]
    for i in range(9, 16):
        ky_part = ky_part + WY[i, 15:16, :]
    ky_part = ky_part * F3[1, 15:16, :] * F3[1, 16:17, :]

    lane8 = lax.broadcasted_iota(jnp.int32, (8, NL), 1)
    sub8 = lax.broadcasted_iota(jnp.int32, (8, NL), 0)

    def solve(m):
        parts = [[jnp.zeros((8, NL), F32) for _ in range(2)] for _ in range(4)]
        for l in range(64):
            value = jnp.broadcast_to(m[:, l : l + 1], (8, NL))
            for c in range(l // 16, 4):
                parts[c][l % 2] += value * KT[8 * l : 8 * l + 8, NL * c : NL * c + NL]
        t = [jnp.broadcast_to(fold(a + b), (8, NL)) for a, b in parts]
        y = jnp.zeros((8, NL), F32)
        for l in range(64):
            p = None
            for c in range(l // 16, 4):
                q = t[c] * KT[8 * l : 8 * l + 8, NL * c : NL * c + NL]
                p = q if p is None else p + q
            s = jnp.broadcast_to(jnp.sum(p, axis=1, keepdims=True), (8, NL))
            YB[8 * l : 8 * l + 8, :] = s
            y = jnp.where(lane8 == l, s, y)
        return y

    def y_at(dx, dy, dz):
        def held(i, d, n):
            return jnp.clip(i + d, 0, n - 1)

        b = (held(ix, dx, n_x) * n_y + held(iy, dy, n_y)) * n_z + held(iz, dz, n_z)
        return YB[pl.ds(b, 1), :]

    def spread():
        for dx in (-1, 0, 1):
            put(FY3, dx + 1, each(jnp.multiply, get(F3, dx + 1), blockwise(y_at, dx)))

    arrived(2, MZ.at[0 : n_z - 1])
    sums0 = jnp.concatenate([MZ[k] + MZ[k + 8] for k in range(8)], axis=0)
    solve(sums0 * (1.0 / 16384.0))
    spread()

    def add_coarse(i):
        put(D0, i, each(jnp.add, get(D0, i), get(FY3, i // 8)))

    loop(4, 20, 4, add_coarse)

    def first_image(i):
        q = a_plane(of(D0), i)
        put(Q, i, q)
        put(FI, i, each(jnp.multiply, get(INV, i), q))

    loop(5, 19, 2, first_image)
    correct(Q, 3, 9)
    smooth(Q, V, 7, 17)

    def products(i, carry):
        r, d, q, v = (ref[i, 0:16, :] for ref in (R, D0, Q, V))
        w = own_sum(a_plane(of(V), i))
        new = (r * d, d * q, q, r * v, q * v, v * w, w)
        return tuple(a + b for a, b in zip(carry, new))

    parts = lax.fori_loop(8, 16, products, (zero16,) * 7)
    rows = [fold(p) for p in parts]
    rows += [fold(e_part), fold(kx_part), ky_part, fold(kz_part)]
    turned = gather(message(rows))
    rd, dq, q_sum, rv, qv, vw, w_sum, e_all, kx, ky, kz = (
        turned[8 * k : 8 * k + 8] for k in range(11)
    )
    y = solve(q_sum * (1.0 / 16384.0))
    spread()

    def all_sum(v):
        return jnp.sum(jnp.sum(v, axis=0, keepdims=True), axis=1, keepdims=True)

    up = pltpu.roll(y, 7, 0)
    y_z = jnp.where(sub8 == 7, pltpu.roll(up, NL - 1, 1), up)
    y_y = pltpu.roll(y, NL - 2, 1)
    y_x = pltpu.roll(y, NL - 16, 1)
    jump = kx * (y - y_x) ** 2 + ky * (y - y_y) ** 2 + kz * (y - y_z) ** 2
    p1, p2 = all_sum(rd), all_sum(dq)
    p4 = all_sum(rv + sums0 * y)
    p5 = all_sum(qv + q_sum * y)
    p6 = all_sum(vw + 2.0 * y * w_sum + e_all * y * y + jump)
    alpha = p1 / p2
    inner = p1 - alpha * (p4 + p2) + alpha * alpha * p5
    ratio = inner / p1
    grown = 1.0 + ratio
    curve = grown * grown * p2 - 2.0 * grown * alpha * p5 + alpha * alpha * p6
    alpha2 = inner / curve

    def direction(i):
        put(D1, i, each(
            lambda d, v, s: grown * d - alpha * (v + s), get(D0, i), get(V, i), get(FY3, i // 8)
        ))

    loop(7, 17, 2, direction)

    def finish(i):
        d0, d1, r, q = (ref[i, 0:16, :] for ref in (D0, D1, R, Q))
        image = own_sum(a_plane(of(D1), i))
        sol_ref[i - 8] = alpha * d0 + alpha2 * d1
        res_ref[i - 8] = r - alpha * q - alpha2 * image

    loop(8, 16, 2, finish)

    for group, all_bytes in pending:
        take(send_sem.at[group], all_bytes)


def solution(mesh):
    dims = tuple(mesh.shape[a] for a in ("gx", "gy", "gz"))
    field = pltpu.VMEM((NX, 2 * NR, NL), F32)
    coarse = pltpu.VMEM((NX // 2, 2 * NR, NL), F32)
    three = pltpu.VMEM((3, 2 * NR, NL), F32)
    sems = pltpu.SemaphoreType.DMA

    def on_device(right_side, conductance, extents, coarse_factor):
        shape = jax.ShapeDtypeStruct((8, 16, 128), F32)
        return pl.pallas_call(
            functools.partial(kernel, dims),
            out_shape=(shape, shape),
            in_specs=[
                pl.BlockSpec(memory_space=pltpu.VMEM),
                pl.BlockSpec(memory_space=pltpu.VMEM),
                pl.BlockSpec(memory_space=pltpu.SMEM),
                pl.BlockSpec(memory_space=pl.ANY),
            ],
            out_specs=(
                pl.BlockSpec(memory_space=pltpu.VMEM),
                pl.BlockSpec(memory_space=pltpu.VMEM),
            ),
            scratch_shapes=[
                *([field] * 12), coarse, coarse, three, three, three,
                pltpu.VMEM((512, 512), F32),
                pltpu.VMEM((512, 512), jnp.bfloat16),
                pltpu.VMEM((512, NL), F32),
                pltpu.VMEM((NL, NL), F32),
                pltpu.VMEM((27, 1, NL), F32),
                pltpu.VMEM((2, 3, 8, NL), F32),
                pltpu.VMEM((2, 9, 3, 8, NL), F32),
                pltpu.VMEM((16, 1, NL), F32),
                pltpu.VMEM((8, 2, NL), F32),
                pltpu.VMEM((4, 8, 2, NL), F32),
                pltpu.VMEM((4, 1, NL), F32),
                pltpu.VMEM((8, 1, NL), F32),
                pltpu.VMEM((16, 1, NL), F32),
                sems(()),
                sems((10,)), sems((10,)),
            ],
            compiler_params=pltpu.CompilerParams(collective_id=0, has_side_effects=True),
        )(right_side, conductance, extents, coarse_factor)

    spec = P("gx", "gy", "gz")
    return jax.shard_map(
        on_device, mesh=mesh, in_specs=(spec, spec, spec, P()), out_specs=(spec, spec),
        check_vma=False,
    )
```

```python
import functools

import jax
import jax.numpy as jnp
from jax import lax
from jax.experimental import pallas as pl
from jax.experimental.pallas import tpu as pltpu
from jax.sharding import PartitionSpec as P

MESH = pl.DeviceIdType.MESH
F32, BF16 = jnp.float32, jnp.bfloat16
NX, NR, NL = 24, 32, 128
ROWS = 80
UNROLL = 24
OWN = slice(16, 32)
SLOTS = [(dx, dy, dz) for dx in (-1, 0, 1) for dy in (-1, 0, 1) for dz in (-1, 0, 1)]
AROUND = [d for d in SLOTS if d != (0, 0, 0)]
PLANAR = [d for d in AROUND if d[2] == 0]
DEEP = [d for d in AROUND if d[2] != 0]


def slot(d):
    return (d[0] + 1) * 9 + (d[1] + 1) * 3 + d[2] + 1


def dot(a, b, turned=False):
    dims = (((1,), (1 if turned else 0,)), ((), ()))
    return lax.dot_general(a, b, dims, preferred_element_type=F32)


def three(x):
    a = x.astype(BF16)
    rest = x - a.astype(F32)
    b = rest.astype(BF16)
    return a, b, (rest - b.astype(F32)).astype(BF16)


def dot_turned(x, m):
    n = x.shape[0]
    p = dot(jnp.concatenate(three(x), axis=0), m, True)
    return p[0:n] + (p[n : 2 * n] + p[2 * n :])


def dot_wide(x, y):
    n = x.shape[0]
    (a, b, c), (d, e, f) = three(x), three(y)
    p = dot(jnp.concatenate([a, b, c], axis=0), d)
    q = dot(jnp.concatenate([a, b], axis=0), e)
    return p[0:n] + ((p[n : 2 * n] + q[0:n]) + (p[2 * n :] + q[n:] + dot(a, f)))


def loop(low, high, unroll, body):
    if unroll >= high - low:
        for i in range(low, high):
            body(i)
        return

    def step(k, carry):
        for u in range(unroll):
            body(low + k * unroll + u)
        return carry

    whole = (high - low) // unroll
    lax.fori_loop(0, whole, step, 0)
    for i in range(low + whole * unroll, high):
        body(i)


def kernel(
    dims, rs_ref, c_ref, ext_ref, l_hbm, sol_ref, res_ref,
    R, C, WX, WY, WZ, INV, FI, SEC, V, D0, Q, D1, C1, INV1, F3, F13, FY3,
    KT, LB, YB, G, XT, ZS, ZR, RZ, RY, RX, MX, MY, MZ,
    l_sem, send_sem, recv_sem,
):
    n_x, n_y, n_z = dims
    ix, iy, iz = (lax.axis_index(a) for a in ("gx", "gy", "gz"))

    def peer(dx, dy, dz):
        return {
            "gx": lax.rem(ix + dx + n_x, n_x),
            "gy": lax.rem(iy + dy + n_y, n_y),
            "gz": lax.rem(iz + dz + n_z, n_z),
        }

    l_copy = pltpu.make_async_copy(l_hbm, LB, l_sem)
    l_copy.start()

    greet = list(AROUND)
    greet += [(0, 0, o) for o in range(2, n_z - 1)]
    greet += [(0, o, 0) for o in range(2, n_y - 1)]
    greet += [(o, 0, 0) for o in range(2, n_x - 1)]
    barrier = pltpu.get_barrier_semaphore()
    for d in greet:
        pl.semaphore_signal(barrier, inc=1, device_id=peer(*d), device_id_type=MESH)

    lane = lax.broadcasted_iota(jnp.int32, (NR, NL), 1)
    sub = lax.broadcasted_iota(jnp.int32, (NR, NL), 0)
    even_z, even_y = lane % 2 == 0, sub % 2 == 0

    def at_end(n, width):
        return lane[0:n] >= NL - width

    def at_start(n, width):
        return lane[0:n] < width

    def zp(p, width=1):
        a, b = pltpu.roll(p[0], NL - width, 1), pltpu.roll(p[1], NL - width, 1)
        edge = at_end(p[0].shape[0], width)
        return jnp.where(edge, b, a), jnp.where(edge, a, b)

    def zm(p, width=1):
        a, b = pltpu.roll(p[0], width, 1), pltpu.roll(p[1], width, 1)
        edge = at_start(p[0].shape[0], width)
        return jnp.where(edge, b, a), jnp.where(edge, a, b)

    def get(ref, i, off=0, own=False):
        start, n = (16 + off, 16) if own else (8 + off, NR)
        return ref[i, start : start + n, :], ref[i, start + NR : start + NR + n, :]

    def put(ref, i, p):
        ref[i, 8 : 8 + NR, :] = p[0]
        ref[i, 8 + NR : 8 + 2 * NR, :] = p[1]

    def each(f, *ps):
        return tuple(f(*(p[h] for p in ps)) for h in range(2))

    def pair_y(v):
        return v + jnp.where(even_y, pltpu.roll(v, NR - 1, 0), pltpu.roll(v, 1, 0))

    def pair_z(v, op=jnp.add):
        return op(v, jnp.where(even_z, pltpu.roll(v, NL - 1, 1), pltpu.roll(v, 1, 1)))

    def of(ref):
        return lambda i, off, own: get(ref, i, off, own)

    def fluid(i, off, own):
        return get(F3, i // 8, off, own)

    def a_plane(v_of, i, own=False):
        v, vp, vm = (v_of(i + k, 0, own) for k in (0, 1, -1))
        up, down = v_of(i, 1, own), v_of(i, -1, own)
        wx, wxm = get(WX, i, 0, own), get(WX, i - 1, 0, own)
        wy, wym, wz = get(WY, i, 0, own), get(WY, i, -1, own), get(WZ, i, 0, own)
        fz = each(lambda w, a, b: w * (a - b), wz, v, zp(v))
        return each(
            lambda f, w, wm, u, um, a, ap, am, ay, aym, h, hm: f * (
                (w * (a - ap) + wm * (a - am)) + (u * (a - ay) + um * (a - aym)) + (h - hm)
            ),
            fluid(i, 0, own), wx, wxm, wy, wym, v, vp, vm, up, down, fz, zm(fz),
        )

    extent = jnp.full((1, NL), ext_ref[0, 0, 0].astype(F32))
    XT[13] = extent
    row16 = lax.broadcasted_iota(jnp.int32, (16, NL), 0)
    lane16 = lax.broadcasted_iota(jnp.int32, (16, NL), 1)
    own_fluid = (lane16.astype(F32) < extent).astype(F32)
    total = jnp.zeros((16, NL), F32)
    for i in range(8):
        r = own_fluid * rs_ref[i]
        R[8 + i, OWN, :] = r
        total = total + r
        C[8 + i, OWN, :] = c_ref[i]

    izlo = lax.rem(iz, 8)

    def message(rows):
        t = jnp.zeros((16, NL), F32)
        for k, row in enumerate(rows):
            t = jnp.where(row16 == k, row, t)
        reduced = jnp.sum(t, axis=1, keepdims=True)
        placed = jnp.where(lane16 == row16 * 8 + izlo, reduced, 0.0)
        return jnp.sum(placed, axis=0, keepdims=True)

    def fold(v):
        return jnp.sum(v, axis=0, keepdims=True)

    pending = []

    def send(src, dst, group, to):
        pltpu.make_async_remote_copy(
            src_ref=src, dst_ref=dst, send_sem=send_sem.at[group], recv_sem=recv_sem.at[group],
            device_id=to, device_id_type=MESH,
        ).start()

    def take(sem, all_bytes):
        pltpu.make_async_copy(all_bytes, all_bytes, sem).wait()

    def arrived(group, all_bytes):
        take(recv_sem.at[group], all_bytes)
        pending.append((group, all_bytes))

    def far_first(n):
        return sorted(range(1, n), key=lambda o: -min(o, n - o))

    def row_stage(group, ref, at, row, n, direction):
        ref[at] = row
        for o in far_first(n):
            send(ref.at[at], ref.at[at], group, peer(*direction(o)))

    def added(ref, n):
        row = ref[0]
        for k in range(1, n):
            row = row + ref[k]
        return row

    def gather(row):
        row_stage(3, RZ, iz, row, n_z, lambda o: (0, 0, o))
        arrived(3, RZ.at[0 : n_z - 1])
        low, high = RZ[0], RZ[8]
        for k in range(1, 8):
            low, high = low + RZ[k], high + RZ[8 + k]
        RY[iy, 0:1, :] = low
        RY[iy, 1:2, :] = high
        for o in far_first(n_y):
            send(RY.at[iy], RY.at[iy], 4, peer(0, o, 0))
        arrived(4, RY.at[0 : n_y - 1])
        RX[ix] = RY[...]
        for o in far_first(n_x):
            send(RY, RX.at[ix], 5, peer(o, 0, 0))
        arrived(5, RX.at[0 : n_x - 1])
        for a in range(n_x):
            for b in range(n_y):
                at = (a * n_y + b) * 2
                G[at : at + 2, :] = RX[a, b]
        return G[...].T

    column = (ix * n_y + iy) * 2 + iz // 8
    lane1 = lax.broadcasted_iota(jnp.int32, (1, NL), 1)
    first_row = jnp.where(lane1 == column, jnp.sum(fold(total), axis=1, keepdims=True), 0.0)
    pl.semaphore_wait(barrier, len(greet))
    row_stage(0, MX, ix, first_row, n_x, lambda o: (o, 0, 0))

    for d in PLANAR:
        dx, dy, _ = d
        to_x = {1: slice(0, 8), -1: slice(16, 24), 0: slice(8, 16)}[dx]
        from_y = {1: slice(24, 32), -1: slice(16, 24), 0: OWN}[dy]
        to_y = {1: slice(8, 16), -1: slice(32, 40), 0: OWN}[dy]
        for group, ref in ((6, C), (7, R)):
            send(ref.at[8:16, from_y, :], ref.at[to_x, to_y, :], group, peer(*d))
        send(XT.at[13], XT.at[slot((-dx, -dy, 0))], 8, peer(*d))
    r_turned = R[8:16, OWN, :].reshape(128, 128).T
    c_turned = c_ref[...].reshape(128, 128).T
    for h, at in ((0, 0), (1, 120)):
        ZS[h, 0] = r_turned[at : at + 8]
        ZS[h, 1] = c_turned[at : at + 8]
        ZS[h, 2] = jnp.broadcast_to(extent, (8, NL))
    for d in DEEP:
        dx, dy, dz = d
        half = (dz + 1) // 2
        send(ZS.at[half], ZR.at[1 - half, (1 - dx) * 3 + 1 - dy], 9, peer(*d))

    l_copy.wait()
    KT[...] = jnp.zeros_like(KT)
    row = lax.broadcasted_iota(jnp.int32, (128, 128), 0)
    col = lax.broadcasted_iota(jnp.int32, (128, 128), 1)
    eye = row == col
    for b in range(4):
        at = slice(128 * b, 128 * b + 128)
        block = LB[at, at].astype(F32)
        KT[at, at] = jnp.where(eye, 1.0 / jnp.where(eye, block, 1.0), 0.0)

    def level(k):
        mask = (row // (2 << k) == col // (2 << k)) & (row // (1 << k) > col // (1 << k))
        for b in range(4):
            at = slice(128 * b, 128 * b + 128)
            m = jnp.where(mask, LB[at, at].astype(F32), 0.0).astype(BF16)
            kt = KT[at, at]
            KT[at, at] = kt - dot_wide(dot_turned(kt, m), kt)

    def join(a, b, w):
        up, down = slice(a, a + w), slice(b, b + w)
        KT[up, down] = -dot_wide(dot_turned(KT[up, up], LB[down, up]), KT[down, down])

    for k in range(4):
        level(k)
    arrived(0, MX.at[0 : n_x - 1])
    row_stage(1, MY, iy, added(MX, n_x), n_y, lambda o: (0, o, 0))
    for k in range(4, 7):
        level(k)
    join(0, 128, 128)
    join(256, 384, 128)
    join(0, 256, 256)
    G[64:128, :] = jnp.zeros((64, NL), F32)
    arrived(1, MY.at[0 : n_y - 1])
    row_stage(2, MZ, iz, added(MY, n_y), n_z, lambda o: (0, 0, o))

    arrived(6, C.at[0:8])
    arrived(7, R.at[0:8])
    arrived(8, XT.at[0:8])
    arrived(9, ZR)

    def there(dx, dy, dz):
        ok = None
        for d, i, n in ((dx, ix, n_x), (dy, iy, n_y), (dz, iz, n_z)):
            if d:
                test = i + d >= 0 if d < 0 else i + d < n
                ok = test if ok is None else ok & test
        return jnp.float32(1.0) if ok is None else ok.astype(F32)

    def blockwise(value, dx):
        lower = sub < 8
        middle = sub < 24
        near = [value(dx, dy, 0) for dy in (-1, 0, 1)]
        above = [value(dx, dy, 1) for dy in (-1, 0, 1)]
        below = [value(dx, dy, -1) for dy in (-1, 0, 1)]
        by_y = [jnp.where(lower, a, jnp.where(middle, b, c)) for a, b, c in (near, above, below)]
        return by_y[0], jnp.where(lane < 64, by_y[1], by_y[2])

    def extent_at(dx, dy, dz):
        if dz == 0:
            e = XT[slot((dx, dy, dz))]
        else:
            e = ZR[(dz + 1) // 2, (dx + 1) * 3 + dy + 1, 2, 0:1, :]
        return e * there(dx, dy, dz)

    lane_f = lane.astype(F32)
    for dx in (-1, 0, 1):
        f = each(lambda e: (lane_f < e).astype(F32), blockwise(extent_at, dx))
        put(F3, dx + 1, f)
        put(F13, dx + 1, each(lambda a: pair_z(a, jnp.maximum), f))

    blank = jnp.zeros((104 + 8, NL), F32)
    for dx in (-1, 0, 1):
        to_x = 8 + 8 * dx
        for dy in (-1, 0, 1):
            from_y = {1: 0, -1: 8, 0: 0}[dy]
            to_y = 8 + NR + {1: 24, -1: 0, 0: 8}[dy]
            wide = 16 if dy == 0 else 8
            at = (dx + 1) * 3 + dy + 1
            above, below = there(dx, dy, 1), there(dx, dy, -1)
            for f, ref in enumerate((R, C)):
                t = jnp.concatenate([ZR[1, at, f] * above, blank, ZR[0, at, f] * below], axis=0).T
                t = t.reshape(8, 16, NL)
                ref[to_x : to_x + 8, to_y : to_y + wide, :] = t[:, from_y : from_y + wide, :]

    @pl.when(ix == 0)
    def _():
        C[0:8, 8:40, :] = jnp.zeros((8, NR, NL), F32)

    @pl.when(ix == n_x - 1)
    def _():
        C[16:24, 8:40, :] = jnp.zeros((8, NR, NL), F32)

    @pl.when(iy == n_y - 1)
    def _():
        C[:, 32:40, :] = jnp.zeros((NX, 8, NL), F32)

    @pl.when(iy == 0)
    def _():
        C[:, 8:16, :] = jnp.zeros((NX, 8, NL), F32)

    def coefficients(i):
        c, cp, cm = get(C, i), get(C, i + 1), get(C, i - 1)
        half = lambda a, b: 0.5 * (a + b)
        wx, wxm = each(half, c, cp), each(half, c, cm)
        wy, wym = each(half, c, get(C, i, 1)), each(half, c, get(C, i, -1))
        wz, wzm = each(half, c, zp(c)), each(half, c, zm(c))
        inv = each(
            lambda a, am, b, bm, z, m, g: 0.8 * g / ((a + am) + (b + bm) + (z + m) + 1.0 - g),
            wx, wxm, wy, wym, wz, wzm, fluid(i, 0, False),
        )
        put(WX, i, wx)
        put(WY, i, wy)
        put(WZ, i, wz)
        put(INV, i, inv)
        put(FI, i, each(jnp.multiply, inv, get(R, i)))

    loop(1, 23, UNROLL, coefficients)

    def pool(a, b):
        return each(lambda u, v: pair_z(pair_y(u + v)), a, b)

    def coarse_mean(j):
        put(C1, j, each(lambda a: a * 0.125, pool(get(C, 2 * j), get(C, 2 * j + 1))))

    loop(0, 12, UNROLL, coarse_mean)

    def coarse_inverse(j):
        c = get(C1, j)
        put(INV1, j, each(
            lambda a, p, m, u, d, g, h, e: 0.8 * e / (
                2.0 * (6.0 * a + (p + m) + (u + d) + (g + h)) + 1.0 - e
            ),
            c, get(C1, j + 1), get(C1, j - 1), get(C1, j, 2), get(C1, j, -2), zp(c, 2), zm(c, 2),
            get(F13, j // 4),
        ))

    loop(1, 11, UNROLL, coarse_inverse)

    def correct(src, low, high):
        def body(j):
            rest = [
                each(jnp.subtract, get(src, i), a_plane(of(FI), i)) for i in (2 * j, 2 * j + 1)
            ]
            below = each(jnp.multiply, get(INV1, j), pool(*rest))
            shift = each(jnp.multiply, get(F3, j // 4), below)
            for i in (2 * j, 2 * j + 1):
                put(SEC, i, each(jnp.add, get(FI, i), shift))

        loop(low, high, UNROLL, body)

    def smooth(src, dst, low, high):
        def body(i):
            put(dst, i, each(
                lambda s, w, r, a: s + w * (r - a),
                get(SEC, i), get(INV, i), get(src, i), a_plane(of(SEC), i),
            ))

        loop(low, high, UNROLL, body)

    correct(R, 1, 11)
    smooth(R, D0, 4, 20)

    f_own = get(F3, 1, 0, True)
    fn_own = zp(f_own)
    e_part = kz_part = jnp.zeros((16, NL), F32)
    for i in range(8, 16):
        e_part = e_part + a_plane(fluid, i, True)[0]
        kz_part = kz_part + WZ[i, OWN, :]
    kz_part = jnp.where(lane16 == NL - 1, kz_part * f_own[0] * fn_own[0], 0.0)
    kx_part = WX[15, OWN, :] * F3[1, OWN, :] * F3[2, OWN, :]
    ky_part = WY[8, 31:32, :]
    for i in range(9, 16):
        ky_part = ky_part + WY[i, 31:32, :]
    ky_part = ky_part * F3[1, 31:32, :] * F3[1, 32:33, :]

    lane8 = lax.broadcasted_iota(jnp.int32, (8, NL), 1)
    sub8 = lax.broadcasted_iota(jnp.int32, (8, NL), 0)

    def solve(m):
        parts = [[jnp.zeros((8, NL), F32) for _ in range(2)] for _ in range(4)]
        for l in range(64):
            value = jnp.broadcast_to(m[:, l : l + 1], (8, NL))
            for c in range(l // 16, 4):
                parts[c][l % 2] += value * KT[8 * l : 8 * l + 8, NL * c : NL * c + NL]
        t = [jnp.broadcast_to(fold(a + b), (8, NL)) for a, b in parts]
        y = jnp.zeros((8, NL), F32)
        for l in range(64):
            p = None
            for c in range(l // 16, 4):
                q = t[c] * KT[8 * l : 8 * l + 8, NL * c : NL * c + NL]
                p = q if p is None else p + q
            s = jnp.broadcast_to(jnp.sum(p, axis=1, keepdims=True), (8, NL))
            YB[8 * l : 8 * l + 8, :] = s
            y = jnp.where(lane8 == l, s, y)
        return y

    def y_at(dx, dy, dz):
        def held(i, d, n):
            return jnp.clip(i + d, 0, n - 1)

        b = (held(ix, dx, n_x) * n_y + held(iy, dy, n_y)) * n_z + held(iz, dz, n_z)
        return YB[pl.ds(b, 1), :]

    def spread():
        for dx in (-1, 0, 1):
            put(FY3, dx + 1, each(jnp.multiply, get(F3, dx + 1), blockwise(y_at, dx)))

    arrived(2, MZ.at[0 : n_z - 1])
    sums0 = jnp.concatenate([MZ[k] + MZ[k + 8] for k in range(8)], axis=0)
    solve(sums0 * (1.0 / 16384.0))
    spread()

    def add_coarse(i):
        put(D0, i, each(jnp.add, get(D0, i), get(FY3, i // 8)))

    loop(4, 20, UNROLL, add_coarse)

    def first_image(i):
        q = a_plane(of(D0), i)
        put(Q, i, q)
        put(FI, i, each(jnp.multiply, get(INV, i), q))

    loop(5, 19, UNROLL, first_image)
    correct(Q, 3, 9)
    smooth(Q, V, 7, 17)

    parts = [None] * 7
    for i in range(8, 16):
        r, d, q, v = (ref[i, OWN, :] for ref in (R, D0, Q, V))
        w = a_plane(of(V), i, True)[0]
        new = (r * d, d * q, q, r * v, q * v, v * w, w)
        parts = [b if a is None else a + b for a, b in zip(parts, new)]

    rows = [fold(p) for p in parts]
    rows += [fold(e_part), fold(kx_part), ky_part, fold(kz_part)]
    turned = gather(message(rows))
    rd, dq, q_sum, rv, qv, vw, w_sum, e_all, kx, ky, kz = (
        turned[8 * k : 8 * k + 8] for k in range(11)
    )
    y = solve(q_sum * (1.0 / 16384.0))
    spread()

    def all_sum(v):
        return jnp.sum(jnp.sum(v, axis=0, keepdims=True), axis=1, keepdims=True)

    up = pltpu.roll(y, 7, 0)
    y_z = jnp.where(sub8 == 7, pltpu.roll(up, NL - 1, 1), up)
    y_y = pltpu.roll(y, NL - 2, 1)
    y_x = pltpu.roll(y, NL - 16, 1)
    jump = kx * (y - y_x) ** 2 + ky * (y - y_y) ** 2 + kz * (y - y_z) ** 2
    p1, p2 = all_sum(rd), all_sum(dq)
    p4 = all_sum(rv + sums0 * y)
    p5 = all_sum(qv + q_sum * y)
    p6 = all_sum(vw + 2.0 * y * w_sum + e_all * y * y + jump)
    alpha = p1 / p2
    inner = p1 - alpha * (p4 + p2) + alpha * alpha * p5
    ratio = inner / p1
    grown = 1.0 + ratio
    curve = grown * grown * p2 - 2.0 * grown * alpha * p5 + alpha * alpha * p6
    alpha2 = inner / curve

    def direction(i):
        put(D1, i, each(
            lambda d, v, s: grown * d - alpha * (v + s), get(D0, i), get(V, i), get(FY3, i // 8)
        ))

    loop(7, 17, UNROLL, direction)

    for i in range(8, 16):
        d0, d1, r, q = (ref[i, OWN, :] for ref in (D0, D1, R, Q))
        image = a_plane(of(D1), i, True)[0]
        sol_ref[i - 8] = alpha * d0 + alpha2 * d1
        res_ref[i - 8] = r - alpha * q - alpha2 * image

    for group, all_bytes in pending:
        take(send_sem.at[group], all_bytes)


def solution(mesh):
    dims = tuple(mesh.shape[a] for a in ("gx", "gy", "gz"))
    field = pltpu.VMEM((NX, ROWS, NL), F32)
    coarse = pltpu.VMEM((NX // 2, ROWS, NL), F32)
    three = pltpu.VMEM((3, ROWS, NL), F32)
    sems = pltpu.SemaphoreType.DMA

    def on_device(right_side, conductance, extents, coarse_factor):
        shape = jax.ShapeDtypeStruct((8, 16, 128), F32)
        return pl.pallas_call(
            functools.partial(kernel, dims),
            out_shape=(shape, shape),
            in_specs=[
                pl.BlockSpec(memory_space=pltpu.VMEM),
                pl.BlockSpec(memory_space=pltpu.VMEM),
                pl.BlockSpec(memory_space=pltpu.SMEM),
                pl.BlockSpec(memory_space=pl.ANY),
            ],
            out_specs=(
                pl.BlockSpec(memory_space=pltpu.VMEM),
                pl.BlockSpec(memory_space=pltpu.VMEM),
            ),
            scratch_shapes=[
                *([field] * 12), coarse, coarse, three, three, three,
                pltpu.VMEM((512, 512), F32),
                pltpu.VMEM((512, 512), jnp.bfloat16),
                pltpu.VMEM((512, NL), F32),
                pltpu.VMEM((NL, NL), F32),
                pltpu.VMEM((27, 1, NL), F32),
                pltpu.VMEM((2, 3, 8, NL), F32),
                pltpu.VMEM((2, 9, 3, 8, NL), F32),
                pltpu.VMEM((16, 1, NL), F32),
                pltpu.VMEM((8, 2, NL), F32),
                pltpu.VMEM((4, 8, 2, NL), F32),
                pltpu.VMEM((4, 1, NL), F32),
                pltpu.VMEM((8, 1, NL), F32),
                pltpu.VMEM((16, 1, NL), F32),
                sems(()),
                sems((10,)), sems((10,)),
            ],
            compiler_params=pltpu.CompilerParams(collective_id=0, has_side_effects=True),
        )(right_side, conductance, extents, coarse_factor)

    spec = P("gx", "gy", "gz")
    return jax.shard_map(
        on_device, mesh=mesh, in_specs=(spec, spec, spec, P()), out_specs=(spec, spec),
        check_vma=False,
    )
```

```python
import functools

import jax
import jax.numpy as jnp
from jax import lax
from jax.experimental import pallas as pl
from jax.experimental.pallas import tpu as pltpu
from jax.sharding import PartitionSpec as P

MESH = pl.DeviceIdType.MESH
F32, BF16 = jnp.float32, jnp.bfloat16
NX, NR, NL = 24, 32, 128
ROWS = 80
UNROLL = 24
VMEM_LIMIT = 24 << 20
OWN = slice(16, 32)
SLOTS = [(dx, dy, dz) for dx in (-1, 0, 1) for dy in (-1, 0, 1) for dz in (-1, 0, 1)]
AROUND = [d for d in SLOTS if d != (0, 0, 0)]
PLANAR = [d for d in AROUND if d[2] == 0]
DEEP = [d for d in AROUND if d[2] != 0]


def slot(d):
    return (d[0] + 1) * 9 + (d[1] + 1) * 3 + d[2] + 1


def dot(a, b, turned=False):
    dims = (((1,), (1 if turned else 0,)), ((), ()))
    return lax.dot_general(a, b, dims, preferred_element_type=F32)


def three(x):
    a = x.astype(BF16)
    rest = x - a.astype(F32)
    b = rest.astype(BF16)
    return a, b, (rest - b.astype(F32)).astype(BF16)


def dot_turned(x, m):
    n = x.shape[0]
    p = dot(jnp.concatenate(three(x), axis=0), m, True)
    return p[0:n] + (p[n : 2 * n] + p[2 * n :])


def dot_wide(x, y):
    n = x.shape[0]
    (a, b, c), (d, e, f) = three(x), three(y)
    p = dot(jnp.concatenate([a, b, c], axis=0), d)
    q = dot(jnp.concatenate([a, b], axis=0), e)
    return p[0:n] + ((p[n : 2 * n] + q[0:n]) + (p[2 * n :] + q[n:] + dot(a, f)))


def loop(low, high, unroll, body):
    if unroll >= high - low:
        for i in range(low, high):
            body(i)
        return

    def step(k, carry):
        for u in range(unroll):
            body(low + k * unroll + u)
        return carry

    whole = (high - low) // unroll
    lax.fori_loop(0, whole, step, 0)
    for i in range(low + whole * unroll, high):
        body(i)


def kernel(
    dims, rs_hbm, c_hbm, ext_ref, l_hbm, sol_ref, res_ref,
    R, C, WX, WY, WZ, INV, FI, SEC, V, D0, Q, D1, C1, INV1, F3, F13, FY3,
    KT, LB, YB, G, XT, ZS, ZR, RZ, RY, RX, MX, MY, MZ, RS,
    in_sem, send_sem, recv_sem,
):
    n_x, n_y, n_z = dims
    ix, iy, iz = (lax.axis_index(a) for a in ("gx", "gy", "gz"))

    def peer(dx, dy, dz):
        return {
            "gx": lax.rem(ix + dx + n_x, n_x),
            "gy": lax.rem(iy + dy + n_y, n_y),
            "gz": lax.rem(iz + dz + n_z, n_z),
        }

    greet = list(AROUND)
    greet += [(0, 0, o) for o in range(2, n_z - 1)]
    greet += [(0, o, 0) for o in range(2, n_y - 1)]
    greet += [(o, 0, 0) for o in range(2, n_x - 1)]
    barrier = pltpu.get_barrier_semaphore()
    for d in greet:
        pl.semaphore_signal(barrier, inc=1, device_id=peer(*d), device_id_type=MESH)

    rs_copy = pltpu.make_async_copy(rs_hbm, RS, in_sem.at[0])
    c_copy = pltpu.make_async_copy(c_hbm, C.at[8:16, OWN, :], in_sem.at[1])
    l_copy = pltpu.make_async_copy(l_hbm, LB, in_sem.at[2])
    rs_copy.start()
    c_copy.start()
    l_copy.start()

    lane = lax.broadcasted_iota(jnp.int32, (NR, NL), 1)
    sub = lax.broadcasted_iota(jnp.int32, (NR, NL), 0)
    even_z, even_y = lane % 2 == 0, sub % 2 == 0

    def at_end(n, width):
        return lane[0:n] >= NL - width

    def at_start(n, width):
        return lane[0:n] < width

    def zp(p, width=1):
        a, b = pltpu.roll(p[0], NL - width, 1), pltpu.roll(p[1], NL - width, 1)
        edge = at_end(p[0].shape[0], width)
        return jnp.where(edge, b, a), jnp.where(edge, a, b)

    def zm(p, width=1):
        a, b = pltpu.roll(p[0], width, 1), pltpu.roll(p[1], width, 1)
        edge = at_start(p[0].shape[0], width)
        return jnp.where(edge, b, a), jnp.where(edge, a, b)

    def get(ref, i, off=0, own=False):
        start, n = (16 + off, 16) if own else (8 + off, NR)
        return ref[i, start : start + n, :], ref[i, start + NR : start + NR + n, :]

    def put(ref, i, p):
        ref[i, 8 : 8 + NR, :] = p[0]
        ref[i, 8 + NR : 8 + 2 * NR, :] = p[1]

    def each(f, *ps):
        return tuple(f(*(p[h] for p in ps)) for h in range(2))

    def pair_y(v):
        return v + jnp.where(even_y, pltpu.roll(v, NR - 1, 0), pltpu.roll(v, 1, 0))

    def pair_z(v, op=jnp.add):
        return op(v, jnp.where(even_z, pltpu.roll(v, NL - 1, 1), pltpu.roll(v, 1, 1)))

    def of(ref):
        return lambda i, off, own: get(ref, i, off, own)

    def fluid(i, off, own):
        return get(F3, i // 8, off, own)

    def a_plane(v_of, i, own=False):
        v, vp, vm = (v_of(i + k, 0, own) for k in (0, 1, -1))
        up, down = v_of(i, 1, own), v_of(i, -1, own)
        wx, wxm = get(WX, i, 0, own), get(WX, i - 1, 0, own)
        wy, wym, wz = get(WY, i, 0, own), get(WY, i, -1, own), get(WZ, i, 0, own)
        fz = each(lambda w, a, b: w * (a - b), wz, v, zp(v))
        return each(
            lambda f, w, wm, u, um, a, ap, am, ay, aym, h, hm: f * (
                (w * (a - ap) + wm * (a - am)) + (u * (a - ay) + um * (a - aym)) + (h - hm)
            ),
            fluid(i, 0, own), wx, wxm, wy, wym, v, vp, vm, up, down, fz, zm(fz),
        )

    extent = jnp.full((1, NL), ext_ref[0, 0, 0].astype(F32))
    XT[13] = extent
    row16 = lax.broadcasted_iota(jnp.int32, (16, NL), 0)
    lane16 = lax.broadcasted_iota(jnp.int32, (16, NL), 1)
    own_fluid = (lane16.astype(F32) < extent).astype(F32)
    total = jnp.zeros((16, NL), F32)
    rs_copy.wait()
    for i in range(8):
        r = own_fluid * RS[i]
        R[8 + i, OWN, :] = r
        total = total + r

    izlo = lax.rem(iz, 8)

    def message(rows):
        t = jnp.zeros((16, NL), F32)
        for k, row in enumerate(rows):
            t = jnp.where(row16 == k, row, t)
        reduced = jnp.sum(t, axis=1, keepdims=True)
        placed = jnp.where(lane16 == row16 * 8 + izlo, reduced, 0.0)
        return jnp.sum(placed, axis=0, keepdims=True)

    def fold(v):
        return jnp.sum(v, axis=0, keepdims=True)

    pending = []

    def send(src, dst, group, to):
        pltpu.make_async_remote_copy(
            src_ref=src, dst_ref=dst, send_sem=send_sem.at[group], recv_sem=recv_sem.at[group],
            device_id=to, device_id_type=MESH,
        ).start()

    def take(sem, all_bytes):
        pltpu.make_async_copy(all_bytes, all_bytes, sem).wait()

    def arrived(group, all_bytes):
        take(recv_sem.at[group], all_bytes)
        pending.append((group, all_bytes))

    def far_first(n):
        return sorted(range(1, n), key=lambda o: -min(o, n - o))

    def row_stage(group, ref, at, row, n, direction):
        ref[at] = row
        for o in far_first(n):
            send(ref.at[at], ref.at[at], group, peer(*direction(o)))

    def added(ref, n):
        row = ref[0]
        for k in range(1, n):
            row = row + ref[k]
        return row

    def gather(row):
        row_stage(3, RZ, iz, row, n_z, lambda o: (0, 0, o))
        arrived(3, RZ.at[0 : n_z - 1])
        low, high = RZ[0], RZ[8]
        for k in range(1, 8):
            low, high = low + RZ[k], high + RZ[8 + k]
        RY[iy, 0:1, :] = low
        RY[iy, 1:2, :] = high
        for o in far_first(n_y):
            send(RY.at[iy], RY.at[iy], 4, peer(0, o, 0))
        arrived(4, RY.at[0 : n_y - 1])
        RX[ix] = RY[...]
        for o in far_first(n_x):
            send(RY, RX.at[ix], 5, peer(o, 0, 0))
        arrived(5, RX.at[0 : n_x - 1])
        for a in range(n_x):
            for b in range(n_y):
                at = (a * n_y + b) * 2
                G[at : at + 2, :] = RX[a, b]
        return G[...].T

    column = (ix * n_y + iy) * 2 + iz // 8
    lane1 = lax.broadcasted_iota(jnp.int32, (1, NL), 1)
    first_row = jnp.where(lane1 == column, jnp.sum(fold(total), axis=1, keepdims=True), 0.0)
    c_copy.wait()
    pl.semaphore_wait(barrier, len(greet))
    row_stage(0, MX, ix, first_row, n_x, lambda o: (o, 0, 0))

    for d in PLANAR:
        dx, dy, _ = d
        to_x = {1: slice(0, 8), -1: slice(16, 24), 0: slice(8, 16)}[dx]
        from_y = {1: slice(24, 32), -1: slice(16, 24), 0: OWN}[dy]
        to_y = {1: slice(8, 16), -1: slice(32, 40), 0: OWN}[dy]
        for group, ref in ((6, C), (7, R)):
            send(ref.at[8:16, from_y, :], ref.at[to_x, to_y, :], group, peer(*d))
        send(XT.at[13], XT.at[slot((-dx, -dy, 0))], 8, peer(*d))
    r_turned = R[8:16, OWN, :].reshape(128, 128).T
    c_turned = C[8:16, OWN, :].reshape(128, 128).T
    for h, at in ((0, 0), (1, 120)):
        ZS[h, 0] = r_turned[at : at + 8]
        ZS[h, 1] = c_turned[at : at + 8]
        ZS[h, 2] = jnp.broadcast_to(extent, (8, NL))
    for d in DEEP:
        dx, dy, dz = d
        half = (dz + 1) // 2
        send(ZS.at[half], ZR.at[1 - half, (1 - dx) * 3 + 1 - dy], 9, peer(*d))

    l_copy.wait()
    KT[...] = jnp.zeros_like(KT)
    row = lax.broadcasted_iota(jnp.int32, (128, 128), 0)
    col = lax.broadcasted_iota(jnp.int32, (128, 128), 1)
    eye = row == col
    for b in range(4):
        at = slice(128 * b, 128 * b + 128)
        block = LB[at, at].astype(F32)
        KT[at, at] = jnp.where(eye, 1.0 / jnp.where(eye, block, 1.0), 0.0)

    def level(k):
        mask = (row // (2 << k) == col // (2 << k)) & (row // (1 << k) > col // (1 << k))
        for b in range(4):
            at = slice(128 * b, 128 * b + 128)
            m = jnp.where(mask, LB[at, at].astype(F32), 0.0).astype(BF16)
            kt = KT[at, at]
            KT[at, at] = kt - dot_wide(dot_turned(kt, m), kt)

    def join(a, b, w):
        up, down = slice(a, a + w), slice(b, b + w)
        KT[up, down] = -dot_wide(dot_turned(KT[up, up], LB[down, up]), KT[down, down])

    for k in range(4):
        level(k)
    arrived(0, MX.at[0 : n_x - 1])
    row_stage(1, MZ, iz, added(MX, n_x), n_z, lambda o: (0, 0, o))
    for k in range(4, 7):
        level(k)
    join(0, 128, 128)
    join(256, 384, 128)
    join(0, 256, 256)
    G[64:128, :] = jnp.zeros((64, NL), F32)
    arrived(1, MZ.at[0 : n_z - 1])
    tile = jnp.concatenate([MZ[k] + MZ[k + 8] for k in range(8)], axis=0)
    row_stage(2, MY, iy, tile, n_y, lambda o: (0, o, 0))

    arrived(6, C.at[0:8])
    arrived(7, R.at[0:8])
    arrived(8, XT.at[0:8])
    arrived(9, ZR)

    def there(dx, dy, dz):
        ok = None
        for d, i, n in ((dx, ix, n_x), (dy, iy, n_y), (dz, iz, n_z)):
            if d:
                test = i + d >= 0 if d < 0 else i + d < n
                ok = test if ok is None else ok & test
        return jnp.float32(1.0) if ok is None else ok.astype(F32)

    def blockwise(value, dx):
        lower = sub < 8
        middle = sub < 24
        near = [value(dx, dy, 0) for dy in (-1, 0, 1)]
        above = [value(dx, dy, 1) for dy in (-1, 0, 1)]
        below = [value(dx, dy, -1) for dy in (-1, 0, 1)]
        by_y = [jnp.where(lower, a, jnp.where(middle, b, c)) for a, b, c in (near, above, below)]
        return by_y[0], jnp.where(lane < 64, by_y[1], by_y[2])

    def extent_at(dx, dy, dz):
        if dz == 0:
            e = XT[slot((dx, dy, dz))]
        else:
            e = ZR[(dz + 1) // 2, (dx + 1) * 3 + dy + 1, 2, 0:1, :]
        return e * there(dx, dy, dz)

    lane_f = lane.astype(F32)
    for dx in (-1, 0, 1):
        f = each(lambda e: (lane_f < e).astype(F32), blockwise(extent_at, dx))
        put(F3, dx + 1, f)
        put(F13, dx + 1, each(lambda a: pair_z(a, jnp.maximum), f))

    blank = jnp.zeros((104 + 8, NL), F32)
    for dx in (-1, 0, 1):
        to_x = 8 + 8 * dx
        for dy in (-1, 0, 1):
            from_y = {1: 0, -1: 8, 0: 0}[dy]
            to_y = 8 + NR + {1: 24, -1: 0, 0: 8}[dy]
            wide = 16 if dy == 0 else 8
            at = (dx + 1) * 3 + dy + 1
            above, below = there(dx, dy, 1), there(dx, dy, -1)
            for f, ref in enumerate((R, C)):
                t = jnp.concatenate([ZR[1, at, f] * above, blank, ZR[0, at, f] * below], axis=0).T
                t = t.reshape(8, 16, NL)
                ref[to_x : to_x + 8, to_y : to_y + wide, :] = t[:, from_y : from_y + wide, :]

    @pl.when(ix == 0)
    def _():
        C[0:8, 8:40, :] = jnp.zeros((8, NR, NL), F32)

    @pl.when(ix == n_x - 1)
    def _():
        C[16:24, 8:40, :] = jnp.zeros((8, NR, NL), F32)

    @pl.when(iy == n_y - 1)
    def _():
        C[:, 32:40, :] = jnp.zeros((NX, 8, NL), F32)

    @pl.when(iy == 0)
    def _():
        C[:, 8:16, :] = jnp.zeros((NX, 8, NL), F32)

    def coefficients(i):
        c, cp, cm = get(C, i), get(C, i + 1), get(C, i - 1)
        half = lambda a, b: 0.5 * (a + b)
        wx, wxm = each(half, c, cp), each(half, c, cm)
        wy, wym = each(half, c, get(C, i, 1)), each(half, c, get(C, i, -1))
        wz, wzm = each(half, c, zp(c)), each(half, c, zm(c))
        inv = each(
            lambda a, am, b, bm, z, m, g: 0.8 * g / ((a + am) + (b + bm) + (z + m) + 1.0 - g),
            wx, wxm, wy, wym, wz, wzm, fluid(i, 0, False),
        )
        put(WX, i, wx)
        put(WY, i, wy)
        put(WZ, i, wz)
        put(INV, i, inv)
        put(FI, i, each(jnp.multiply, inv, get(R, i)))

    loop(1, 23, UNROLL, coefficients)

    def pool(a, b):
        return each(lambda u, v: pair_z(pair_y(u + v)), a, b)

    def coarse_mean(j):
        put(C1, j, each(lambda a: a * 0.125, pool(get(C, 2 * j), get(C, 2 * j + 1))))

    loop(0, 12, UNROLL, coarse_mean)

    def coarse_inverse(j):
        c = get(C1, j)
        put(INV1, j, each(
            lambda a, p, m, u, d, g, h, e: 0.8 * e / (
                2.0 * (6.0 * a + (p + m) + (u + d) + (g + h)) + 1.0 - e
            ),
            c, get(C1, j + 1), get(C1, j - 1), get(C1, j, 2), get(C1, j, -2), zp(c, 2), zm(c, 2),
            get(F13, j // 4),
        ))

    loop(1, 11, UNROLL, coarse_inverse)

    def correct(src, low, high):
        def body(j):
            rest = [
                each(jnp.subtract, get(src, i), a_plane(of(FI), i)) for i in (2 * j, 2 * j + 1)
            ]
            below = each(jnp.multiply, get(INV1, j), pool(*rest))
            shift = each(jnp.multiply, get(F3, j // 4), below)
            for i in (2 * j, 2 * j + 1):
                put(SEC, i, each(jnp.add, get(FI, i), shift))

        loop(low, high, UNROLL, body)

    def smooth(src, dst, low, high):
        def body(i):
            put(dst, i, each(
                lambda s, w, r, a: s + w * (r - a),
                get(SEC, i), get(INV, i), get(src, i), a_plane(of(SEC), i),
            ))

        loop(low, high, UNROLL, body)

    correct(R, 1, 11)
    smooth(R, D0, 4, 20)

    f_own = get(F3, 1, 0, True)
    fn_own = zp(f_own)
    e_part = kz_part = jnp.zeros((16, NL), F32)
    for i in range(8, 16):
        e_part = e_part + a_plane(fluid, i, True)[0]
        kz_part = kz_part + WZ[i, OWN, :]
    kz_part = jnp.where(lane16 == NL - 1, kz_part * f_own[0] * fn_own[0], 0.0)
    kx_part = WX[15, OWN, :] * F3[1, OWN, :] * F3[2, OWN, :]
    ky_part = WY[8, 31:32, :]
    for i in range(9, 16):
        ky_part = ky_part + WY[i, 31:32, :]
    ky_part = ky_part * F3[1, 31:32, :] * F3[1, 32:33, :]

    lane8 = lax.broadcasted_iota(jnp.int32, (8, NL), 1)
    sub8 = lax.broadcasted_iota(jnp.int32, (8, NL), 0)

    def solve(m):
        parts = [[jnp.zeros((8, NL), F32) for _ in range(2)] for _ in range(4)]
        for l in range(64):
            value = jnp.broadcast_to(m[:, l : l + 1], (8, NL))
            for c in range(l // 16, 4):
                parts[c][l % 2] += value * KT[8 * l : 8 * l + 8, NL * c : NL * c + NL]
        t = [jnp.broadcast_to(fold(a + b), (8, NL)) for a, b in parts]
        y = jnp.zeros((8, NL), F32)
        for l in range(64):
            p = None
            for c in range(l // 16, 4):
                q = t[c] * KT[8 * l : 8 * l + 8, NL * c : NL * c + NL]
                p = q if p is None else p + q
            s = jnp.broadcast_to(jnp.sum(p, axis=1, keepdims=True), (8, NL))
            YB[8 * l : 8 * l + 8, :] = s
            y = jnp.where(lane8 == l, s, y)
        return y

    def y_at(dx, dy, dz):
        def held(i, d, n):
            return jnp.clip(i + d, 0, n - 1)

        b = (held(ix, dx, n_x) * n_y + held(iy, dy, n_y)) * n_z + held(iz, dz, n_z)
        return YB[pl.ds(b, 1), :]

    def spread():
        for dx in (-1, 0, 1):
            put(FY3, dx + 1, each(jnp.multiply, get(F3, dx + 1), blockwise(y_at, dx)))

    arrived(2, MY.at[0 : n_y - 1])
    sums0 = added(MY, n_y)
    solve(sums0 * (1.0 / 16384.0))
    spread()

    def add_coarse(i):
        put(D0, i, each(jnp.add, get(D0, i), get(FY3, i // 8)))

    loop(4, 20, UNROLL, add_coarse)

    def first_image(i):
        q = a_plane(of(D0), i)
        put(Q, i, q)
        put(FI, i, each(jnp.multiply, get(INV, i), q))

    loop(5, 19, UNROLL, first_image)
    correct(Q, 3, 9)
    smooth(Q, V, 7, 17)

    parts = [None] * 7
    for i in range(8, 16):
        r, d, q, v = (ref[i, OWN, :] for ref in (R, D0, Q, V))
        w = a_plane(of(V), i, True)[0]
        new = (r * d, d * q, q, r * v, q * v, v * w, w)
        parts = [b if a is None else a + b for a, b in zip(parts, new)]

    rows = [fold(p) for p in parts]
    rows += [fold(e_part), fold(kx_part), ky_part, fold(kz_part)]
    turned = gather(message(rows))
    rd, dq, q_sum, rv, qv, vw, w_sum, e_all, kx, ky, kz = (
        turned[8 * k : 8 * k + 8] for k in range(11)
    )
    y = solve(q_sum * (1.0 / 16384.0))
    spread()

    def all_sum(v):
        return jnp.sum(jnp.sum(v, axis=0, keepdims=True), axis=1, keepdims=True)

    up = pltpu.roll(y, 7, 0)
    y_z = jnp.where(sub8 == 7, pltpu.roll(up, NL - 1, 1), up)
    y_y = pltpu.roll(y, NL - 2, 1)
    y_x = pltpu.roll(y, NL - 16, 1)
    jump = kx * (y - y_x) ** 2 + ky * (y - y_y) ** 2 + kz * (y - y_z) ** 2
    p1, p2 = all_sum(rd), all_sum(dq)
    p4 = all_sum(rv + sums0 * y)
    p5 = all_sum(qv + q_sum * y)
    p6 = all_sum(vw + 2.0 * y * w_sum + e_all * y * y + jump)
    alpha = p1 / p2
    inner = p1 - alpha * (p4 + p2) + alpha * alpha * p5
    ratio = inner / p1
    grown = 1.0 + ratio
    curve = grown * grown * p2 - 2.0 * grown * alpha * p5 + alpha * alpha * p6
    alpha2 = inner / curve

    def direction(i):
        put(D1, i, each(
            lambda d, v, s: grown * d - alpha * (v + s), get(D0, i), get(V, i), get(FY3, i // 8)
        ))

    loop(7, 17, UNROLL, direction)

    for i in range(8, 16):
        d0, d1, r, q = (ref[i, OWN, :] for ref in (D0, D1, R, Q))
        image = a_plane(of(D1), i, True)[0]
        sol_ref[i - 8] = alpha * d0 + alpha2 * d1
        res_ref[i - 8] = r - alpha * q - alpha2 * image

    for group, all_bytes in pending:
        take(send_sem.at[group], all_bytes)


def solution(mesh):
    dims = tuple(mesh.shape[a] for a in ("gx", "gy", "gz"))
    field = pltpu.VMEM((NX, ROWS, NL), F32)
    coarse = pltpu.VMEM((NX // 2, ROWS, NL), F32)
    three = pltpu.VMEM((3, ROWS, NL), F32)
    sems = pltpu.SemaphoreType.DMA

    def kept(x):
        return pltpu.with_memory_space_constraint(x, pltpu.HBM)

    def on_device(right_side, conductance, extents, coarse_factor):
        shape = jax.ShapeDtypeStruct((8, 16, 128), F32)
        return pl.pallas_call(
            functools.partial(kernel, dims),
            out_shape=(shape, shape),
            in_specs=[
                pl.BlockSpec(memory_space=pltpu.HBM),
                pl.BlockSpec(memory_space=pltpu.HBM),
                pl.BlockSpec(memory_space=pltpu.SMEM),
                pl.BlockSpec(memory_space=pltpu.HBM),
            ],
            out_specs=(
                pl.BlockSpec(memory_space=pltpu.VMEM),
                pl.BlockSpec(memory_space=pltpu.VMEM),
            ),
            scratch_shapes=[
                *([field] * 12), coarse, coarse, three, three, three,
                pltpu.VMEM((512, 512), F32),
                pltpu.VMEM((512, 512), jnp.bfloat16),
                pltpu.VMEM((512, NL), F32),
                pltpu.VMEM((NL, NL), F32),
                pltpu.VMEM((27, 1, NL), F32),
                pltpu.VMEM((2, 3, 8, NL), F32),
                pltpu.VMEM((2, 9, 3, 8, NL), F32),
                pltpu.VMEM((16, 1, NL), F32),
                pltpu.VMEM((8, 2, NL), F32),
                pltpu.VMEM((4, 8, 2, NL), F32),
                pltpu.VMEM((4, 1, NL), F32),
                pltpu.VMEM((8, 8, NL), F32),
                pltpu.VMEM((16, 1, NL), F32),
                pltpu.VMEM((8, 16, NL), F32),
                sems((3,)),
                sems((10,)), sems((10,)),
            ],
            compiler_params=pltpu.CompilerParams(
                collective_id=0, has_side_effects=True, vmem_limit_bytes=VMEM_LIMIT
            ),
        )(kept(right_side), kept(conductance), extents, kept(coarse_factor))

    spec = P("gx", "gy", "gz")
    return jax.shard_map(
        on_device, mesh=mesh, in_specs=(spec, spec, spec, P()), out_specs=(spec, spec),
        check_vma=False,
    )
```
